256 devices in a mesh: lon: 16 (over y_hi, z), day: 16 (over x, y_lo, core).
Axes of the slice: x: 4, y: 4 (y_hi: 2, y_lo: 2; y = y_hi * 2 + y_lo), z: 8, core: 2. Of those that a mesh axis runs over, the one named last changes fastest.
Arguments:
- field: bfloat16 [368, 1440, 1024], P('day', 'lon'), may hold values from -6 to 6
Outputs:
- filtered: float32 [368, 1440, 1024], P('day', 'lon')
The draws below stay inside these ranges and needn't reach their ends.
All inputs are finite; a program needn't handle non-finite values.
Results may differ from the reference program's by a relative error of at most 0.0003.
Values may be sent and summed in bfloat16 or wider, within the bound.
A program may use at most 192 MiB of HBM per device.

```python
import jax
import jax.numpy as jnp
from jax import lax

COLS = 1024
LON = 1440
DAYS = 368
DAY_HALF = 15
LON_HALF = 10


def levels(stream_key, extent, cuts, least, top_value):
    def one(position, shards_of):
        draws = jax.random.uniform(jax.random.fold_in(jax.random.fold_in(stream_key, 6), position), (shards_of,), jnp.float32, least / len(cuts), top_value / len(cuts))
        return jnp.repeat(jnp.exp(draws), extent[position] // shards_of).reshape((-1,) + (1,) * (len(extent) - position - 1))

    level = one(*cuts[0])
    for cut in cuts[1:]:
        level = level * one(*cut)
    return level


def centred(stream_key, dims, deviation, reach, shards=(), kind=jnp.bfloat16):
    drawn = jax.random.normal(stream_key, dims, jnp.float32) * deviation
    if len(shards) > 0:
        drawn = levels(stream_key, dims, shards, -0.22, 0.18) * drawn
    return jnp.clip(drawn, min=-reach, max=reach).astype(kind)


def setup_inputs(seed: int = 0) -> dict:
    key_list = jax.random.split(jax.random.key(seed), 2)
    field = centred(key_list[0], (DAYS, LON, COLS), 1.0, 6.0, ((0, 16), (1, 16)))
    return {"field": field}


def running(values, dim, half):
    count = values.shape[dim] - 2 * half
    total = jnp.cumsum(values, axis=dim)
    first = jnp.zeros_like(lax.slice_in_dim(total, 0, 1, axis=dim))
    total = jnp.concatenate([first, total], axis=dim)
    upper = lax.slice_in_dim(total, 2 * half + 1, 2 * half + 1 + count, axis=dim)
    lower = lax.slice_in_dim(total, 0, count, axis=dim)
    return (upper - lower) / (2.0 * half + 1.0)


def wrapped(values, dim, half):
    size = values.shape[dim]
    head = lax.slice_in_dim(values, size - half, size, axis=dim)
    tail = lax.slice_in_dim(values, 0, half, axis=dim)
    return jnp.concatenate([head, values, tail], axis=dim)


def one_block(block):
    values = block.astype(jnp.float32)
    clim = running(wrapped(values, 0, DAY_HALF), 0, DAY_HALF)
    anomaly = values - clim
    return running(wrapped(anomaly, 1, LON_HALF), 1, LON_HALF)


def reference(field):
    width = 128 if COLS % 128 == 0 else COLS
    blocks = COLS // width
    split = field.reshape(DAYS, LON, blocks, width)
    split = jnp.moveaxis(split, 2, 0)
    result = lax.map(one_block, split)
    return jnp.moveaxis(result, 0, 2).reshape(DAYS, LON, COLS)
```

```python
import functools

import jax
import jax.numpy as jnp
from jax import lax
from jax.experimental import pallas as pl
from jax.experimental.pallas import tpu as pltpu
from jax.sharding import PartitionSpec as P

DAY_HALF = 15
LON_HALF = 10
ROWS = 8
RUN = 8
BLOCK = 10
MESH = pl.DeviceIdType.MESH


def plan(lons):
    edges = [
        (0, ROWS, ROWS - 1),
        (lons - ROWS, ROWS, lons - ROWS),
        (ROWS, ROWS, 2 * ROWS - 1),
        (lons - 2 * ROWS, ROWS, lons - 2 * ROWS),
    ]
    middle = []
    for at in range(2 * ROWS, lons - 2 * ROWS, ROWS):
        size = min(ROWS, lons - 2 * ROWS - at)
        middle.append((at, size, at + ROWS - 1 if size == ROWS else None))
    return edges, middle


def hosts(group):
    at, size, rider = group
    if rider is None:
        return at, size
    return (at, size - 1) if rider > at else (at + 1, size - 1)


def grid(rows, cols):
    return (
        lax.broadcasted_iota(jnp.int32, (rows, cols), 0),
        lax.broadcasted_iota(jnp.int32, (rows, cols), 1),
    )


def ones(condition):
    return jnp.where(condition, 1.0, 0.0).astype(jnp.bfloat16)


def band(days, rows, shift):
    day, other = grid(days, rows)
    away = jnp.abs(day - other - shift)
    weight = jnp.where(away <= DAY_HALF, -1.0, 0.0)
    if shift == 0:
        weight = jnp.where(away == 0, 2.0 * DAY_HALF, weight)
    return weight.astype(jnp.bfloat16)


def dot(weight, values):
    return jnp.dot(weight, values, preferred_element_type=jnp.float32)


def kernel(
    counts, x, out, own, far_days, after, before, packed, anomaly,
    edge_own, edge_before, edge_after,
    own_sem, far_send, far_recv, near_send, near_recv, lon_send, lon_recv,
    jump_send, jump_recv, jump_ready,
):
    lons, days, cols = x.shape
    half = LON_HALF
    day_count, lon_count = counts
    day, lon = lax.axis_index("day"), lax.axis_index("lon")
    day_next = lax.rem(day + 1, day_count)
    day_back = lax.rem(day + day_count - 1, day_count)
    lon_next = lax.rem(lon + 1, lon_count)
    lon_back = lax.rem(lon + lon_count - 1, lon_count)
    even = lax.rem(day, 2) == 0
    odd = jnp.logical_not(even)
    far = jnp.where(even, day_back, day_next)
    near = jnp.where(even, day_next, day_back)
    low_jump = lax.rem(lon, RUN) == 0
    high_jump = lax.rem(lon, RUN) == RUN - 1
    jump = jnp.logical_or(low_jump, high_jump)
    peer = jnp.where(high_jump, lon_next, lon_back)
    edges, middle = plan(lons)
    order = edges + middle
    blocks = lons // BLOCK

    def load(b):
        rows = pl.ds(b * BLOCK, BLOCK)
        return pltpu.make_async_copy(x.at[rows], own.at[rows], own_sem.at[b])

    sequence = [0, blocks - 1, 1, blocks - 2, *range(2, blocks - 2)]
    for b in sequence:
        load(b).start()

    barrier = pltpu.get_barrier_semaphore()
    for axis, who in (
        ("day", day_next), ("day", day_back), ("lon", lon_next), ("lon", lon_back),
    ):
        pl.semaphore_signal(barrier, inc=1, device_id={axis: who}, device_id_type=MESH)
    pl.semaphore_wait(barrier, 4)

    @pl.when(jump)
    def _():
        pl.semaphore_signal(
            jump_ready, inc=1, device_id={"day": far}, device_id_type=MESH
        )

    def remote(src, dst, send, recv, to):
        return pltpu.make_async_remote_copy(
            src_ref=src, dst_ref=dst, send_sem=send, recv_sem=recv,
            device_id=to, device_id_type=MESH,
        )

    start = pl.multiple_of(jnp.where(even, 0, ROWS), ROWS)

    def whole(n):
        at, size, _ = order[n]
        rows = pl.ds(at, size)
        return remote(
            x.at[rows, pl.ds(start, ROWS)], far_days.at[rows, pl.ds(0, ROWS)],
            far_send.at[0, n], far_recv.at[0, n], {"day": far},
        )

    def second(n):
        rows = pl.ds(*hosts(order[n]))
        return remote(
            packed.at[rows], far_days.at[rows, pl.ds(ROWS, ROWS)],
            far_send.at[1, n], far_recv.at[1, n], {"day": far},
        )

    def near_even(b):
        rows = pl.ds(b * BLOCK, BLOCK)
        return remote(
            x.at[rows, pl.ds(ROWS, DAY_HALF)], before.at[rows],
            near_send.at[b], near_recv.at[b], {"day": near},
        )

    def near_odd(b):
        rows = pl.ds(b * BLOCK, BLOCK)
        return remote(
            x.at[rows, pl.ds(0, 2 * ROWS)], after.at[rows],
            near_send.at[b], near_recv.at[b], {"day": near},
        )

    edge = pl.ds(jnp.where(high_jump, lons - half, 0), half)
    across = {"lon": peer}
    corner = {"day": far, "lon": peer}

    def jump_even():
        return [
            remote(x.at[edge, pl.ds(ROWS, DAY_HALF)], edge_own.at[:, pl.ds(ROWS, DAY_HALF)],
                   jump_send.at[0], jump_recv.at[0], across),
        ]

    def jump_odd():
        return [
            remote(x.at[edge, pl.ds(0, ROWS)], edge_own.at[:, pl.ds(0, ROWS)],
                   jump_send.at[0], jump_recv.at[0], across),
            remote(x.at[edge, pl.ds(2 * ROWS, days - 2 * ROWS)],
                   edge_own.at[:, pl.ds(2 * ROWS, days - 2 * ROWS)],
                   jump_send.at[1], jump_recv.at[1], across),
        ]

    def corner_even():
        return [
            remote(x.at[edge, pl.ds(0, 2 * ROWS)], edge_after,
                   jump_send.at[2], jump_recv.at[2], corner),
            remote(far_days.at[edge, pl.ds(0, ROWS)], edge_own.at[:, pl.ds(ROWS, ROWS)],
                   jump_send.at[3], jump_recv.at[3], corner),
        ]

    def corner_odd():
        return [
            remote(x.at[edge, pl.ds(ROWS, DAY_HALF)], edge_before,
                   jump_send.at[4], jump_recv.at[4], corner),
            remote(far_days.at[edge, pl.ds(0, ROWS)], edge_own.at[:, pl.ds(0, ROWS)],
                   jump_send.at[5], jump_recv.at[5], corner),
        ]

    def pass_even():
        return remote(edge_own.at[:, pl.ds(ROWS, DAY_HALF)], edge_before,
                      jump_send.at[6], jump_recv.at[6], {"day": near})

    def pass_odd():
        return remote(edge_own.at[:, pl.ds(0, 2 * ROWS)], edge_after,
                      jump_send.at[7], jump_recv.at[7], {"day": near})

    jump_is_even = jnp.logical_and(jump, even)
    jump_is_odd = jnp.logical_and(jump, odd)

    for n in range(len(edges)):
        whole(n).start()

    @pl.when(even)
    def _():
        for b in range(blocks):
            near_even(b).start()

    @pl.when(odd)
    def _():
        for b in range(blocks):
            near_odd(b).start()

    @pl.when(jump)
    def _():
        pl.semaphore_wait(jump_ready, 1)

    @pl.when(jump_is_even)
    def _():
        for copy in jump_even():
            copy.start()
        corner_even()[0].start()

    @pl.when(jump_is_odd)
    def _():
        for copy in jump_odd():
            copy.start()
        corner_odd()[0].start()

    place, col = grid(ROWS, days)
    part = DAY_HALF - ROWS
    first = jnp.where(even, ROWS, 2 * ROWS)
    keep = ones((place < part) & (col == first + place))

    def pack(n):
        at, size = hosts(order[n])
        rider = order[n][2]
        for i in range(size):
            tile = dot(keep, own[at + i])
            if rider is not None:
                ride = ones((place == part) & (col == first + i))
                tile = tile + dot(ride, own[rider])
            packed[at + i] = tile.astype(jnp.bfloat16)

    waited = 0
    for n in range(len(order)):
        at, size, _ = order[n]
        need = 2 if n < 2 else 4 if n < 4 else min(
            blocks, max(4, sequence.index(min((at + size - 1) // BLOCK, blocks - 3)) + 1)
        )
        while waited < need:
            load(sequence[waited]).wait()
            waited += 1
        if n >= len(edges):
            whole(n).start()
        pack(n)
        if n > 0:
            second(n - 1).start()
    while waited < blocks:
        load(sequence[waited]).wait()
        waited += 1
    own_band = band(3 * ROWS, days, 0)
    before_band = band(3 * ROWS, DAY_HALF, -DAY_HALF)
    after_band = band(3 * ROWS, 2 * ROWS, days)
    second(len(order) - 1).start()

    @pl.when(even)
    def _():
        @pl.loop(0, blocks)
        def _(b):
            near_odd(b).wait_recv()
            for i in range(BLOCK):
                l = b * BLOCK + i
                anomaly[l + half] = dot(own_band, own[l]) + dot(after_band, after[l])

    @pl.when(odd)
    def _():
        @pl.loop(0, blocks)
        def _(b):
            near_even(b).wait_recv()
            for i in range(BLOCK):
                l = b * BLOCK + i
                anomaly[l + half] = dot(own_band, own[l]) + dot(before_band, before[l])

    row, other = grid(2 * ROWS, 2 * ROWS)
    way = jnp.where(even, 1, -1)
    far_band = jnp.where(
        ((other - row) * way >= 0) & (other < DAY_HALF), -1.0, 0.0
    ).astype(jnp.bfloat16)
    touched = pl.ds(start, 2 * ROWS)
    lane, source = grid(ROWS, ROWS)

    def daily(n):
        at, size, rider = order[n]
        whole(n).wait_recv()
        second(n).wait_recv()
        if rider is not None:
            host, count = hosts(order[n])
            tile = jnp.zeros((ROWS, cols), jnp.float32)
            for i in range(count):
                take = ones((lane == i) & (source == part))
                tile = tile + dot(take, far_days[host + i, pl.ds(ROWS, ROWS)])
            far_days[rider, pl.ds(ROWS, ROWS)] = tile.astype(jnp.bfloat16)
        for l in range(at, at + size):
            anomaly[l + half, touched] += dot(far_band, far_days[l])

    pieces = [
        (0, ROWS), (lons - ROWS, ROWS), (ROWS, half - ROWS), (lons - half, half - ROWS),
    ]

    def shift(n):
        at, size = pieces[n]
        low = n % 2 == 0
        place = at + half + (lons if low else -lons)
        return remote(
            anomaly.at[pl.ds(at + half, size)], anomaly.at[pl.ds(place, size)],
            lon_send.at[n], lon_recv.at[n], {"lon": lon_back if low else lon_next},
        )

    def advance(n):
        daily(n)
        if 0 < n <= len(edges):
            stays = low_jump if (n - 1) % 2 == 0 else high_jump

            @pl.when(jnp.logical_not(stays))
            def _():
                shift(n - 1).start()

    for n in range(len(edges)):
        advance(n)

    @pl.when(jump_is_even)
    def _():
        corner_even()[1].start()

    @pl.when(jump_is_odd)
    def _():
        corner_odd()[1].start()

    def pass_on():
        @pl.when(jump_is_even)
        def _():
            jump_even()[0].wait_recv()
            corner_odd()[1].wait_recv()
            pass_even().start()

        @pl.when(jump_is_odd)
        def _():
            for copy in jump_odd():
                copy.wait_recv()
            corner_even()[1].wait_recv()
            pass_odd().start()

    def zonal_edges():
        @pl.when(jump)
        def _():
            @pl.when(even)
            def _():
                corner_odd()[0].wait_recv()
                pass_odd().wait_recv()

            @pl.when(odd)
            def _():
                corner_even()[0].wait_recv()
                pass_even().wait_recv()

            to = jnp.where(high_jump, lons + half, 0)
            for i in range(half):
                anomaly[to + i] = (
                    dot(own_band, edge_own[i])
                    + dot(before_band, edge_before[i])
                    + dot(after_band, edge_after[i])
                )

        @pl.when(jnp.logical_not(high_jump))
        def _():
            shift(0).wait_recv()
            shift(2).wait_recv()

        @pl.when(jnp.logical_not(low_jump))
        def _():
            shift(1).wait_recv()
            shift(3).wait_recv()

    scale = 1.0 / ((2 * DAY_HALF + 1) * (2 * half + 1))
    width = 2 * half + 1

    def up_to(lo, hi, total):
        def step(l, total):
            total = total + (anomaly[l + width - 1] - anomaly[l - 1])
            out[l] = (total * scale)[:days]
            return total

        return lax.fori_loop(lo, hi, step, total)

    def back(step, total):
        l = half - 1 - step
        total = total + (anomaly[l] - anomaly[l + width])
        out[l] = (total * scale)[:days]
        return total

    steps = len(order)
    total = None
    done = half
    for n in range(len(edges), steps):
        end = n == steps - 1
        if n == steps - 3:
            pass_on()
        if end:
            zonal_edges()
            lax.fori_loop(0, half, back, first_total)
        advance(n)
        ready = lons if end else order[n][0] + order[n][1] - half
        if ready <= half:
            continue
        if total is None:
            total = lax.fori_loop(
                half,
                half + width,
                lambda l, t: t + anomaly[l],
                jnp.zeros((3 * ROWS, cols), jnp.float32),
            )
            out[half] = (total * scale)[:days]
            first_total = total
            done = half + 1
        total = up_to(done, ready, total)
        done = ready

    for n in range(steps):
        whole(n).wait_send()
        second(n).wait_send()

    @pl.when(even)
    def _():
        for b in range(blocks):
            near_even(b).wait_send()

    @pl.when(odd)
    def _():
        for b in range(blocks):
            near_odd(b).wait_send()

    for n in range(len(pieces)):
        stays = low_jump if n % 2 == 0 else high_jump

        @pl.when(jnp.logical_not(stays))
        def _():
            shift(n).wait_send()

    @pl.when(jump_is_even)
    def _():
        for copy in (*jump_even(), *corner_even(), pass_even()):
            copy.wait_send()

    @pl.when(jump_is_odd)
    def _():
        for copy in (*jump_odd(), *corner_odd(), pass_odd()):
            copy.wait_send()


def local(counts, field):
    days, lons, cols = field.shape
    x = jnp.transpose(field, (1, 0, 2))
    edges, middle = plan(lons)
    steps = len(edges) + len(middle)
    half = LON_HALF
    y = pl.pallas_call(
        functools.partial(kernel, counts),
        out_shape=pltpu.VMEM((lons, days, cols), jnp.float32),
        in_specs=[pl.BlockSpec(memory_space=pltpu.HBM)],
        out_specs=pl.BlockSpec(memory_space=pltpu.VMEM),
        scratch_shapes=[
            pltpu.VMEM((lons, days, cols), jnp.bfloat16),
            pltpu.VMEM((lons, 2 * ROWS, cols), jnp.bfloat16),
            pltpu.VMEM((lons, 2 * ROWS, cols), jnp.bfloat16),
            pltpu.VMEM((lons, DAY_HALF, cols), jnp.bfloat16),
            pltpu.VMEM((lons, ROWS, cols), jnp.bfloat16),
            pltpu.VMEM((lons + 2 * half, 3 * ROWS, cols), jnp.float32),
            pltpu.VMEM((half, days, cols), jnp.bfloat16),
            pltpu.VMEM((half, DAY_HALF, cols), jnp.bfloat16),
            pltpu.VMEM((half, 2 * ROWS, cols), jnp.bfloat16),
            pltpu.SemaphoreType.DMA((lons // BLOCK,)),
            pltpu.SemaphoreType.DMA((2, steps)),
            pltpu.SemaphoreType.DMA((2, steps)),
            pltpu.SemaphoreType.DMA((lons // BLOCK,)),
            pltpu.SemaphoreType.DMA((lons // BLOCK,)),
            pltpu.SemaphoreType.DMA((4,)),
            pltpu.SemaphoreType.DMA((4,)),
            pltpu.SemaphoreType.DMA((8,)),
            pltpu.SemaphoreType.DMA((8,)),
            pltpu.SemaphoreType.REGULAR,
        ],
        compiler_params=pltpu.CompilerParams(
            collective_id=0, has_side_effects=True, vmem_limit_bytes=52 * 1024 * 1024
        ),
    )(x)
    return jnp.transpose(y, (1, 0, 2))


def solution(mesh):
    return jax.shard_map(
        functools.partial(local, (mesh.shape["day"], mesh.shape["lon"])),
        mesh=mesh,
        in_specs=(P("day", "lon", None),),
        out_specs=P("day", "lon", None),
        check_vma=False,
    )
```

```python
import functools

import jax
import jax.numpy as jnp
from jax import lax
from jax.experimental import pallas as pl
from jax.experimental.pallas import tpu as pltpu
from jax.sharding import PartitionSpec as P

DAY_HALF = 15
LON_HALF = 10
ROWS = 8
RUN = 8
BLOCK = 10
MESH = pl.DeviceIdType.MESH


def plan(lons):
    edges = [
        (0, ROWS, ROWS - 1),
        (lons - ROWS, ROWS, lons - ROWS),
        (ROWS, ROWS, 2 * ROWS - 1),
        (lons - 2 * ROWS, ROWS, lons - 2 * ROWS),
    ]
    middle = []
    for at in range(2 * ROWS, lons - 2 * ROWS, ROWS):
        size = min(ROWS, lons - 2 * ROWS - at)
        middle.append((at, size, at + ROWS - 1 if size == ROWS else None))
    return edges, middle


def hosts(group):
    at, size, rider = group
    if rider is None:
        return at, size
    return (at, size - 1) if rider > at else (at + 1, size - 1)


def grid(rows, cols):
    return (
        lax.broadcasted_iota(jnp.int32, (rows, cols), 0),
        lax.broadcasted_iota(jnp.int32, (rows, cols), 1),
    )


def ones(condition):
    return jnp.where(condition, 1.0, 0.0).astype(jnp.bfloat16)


def band(days, rows, shift):
    day, other = grid(days, rows)
    away = jnp.abs(day - other - shift)
    weight = jnp.where(away <= DAY_HALF, -1.0, 0.0)
    if shift == 0:
        weight = jnp.where(away == 0, 2.0 * DAY_HALF, weight)
    return weight.astype(jnp.bfloat16)


def dot(weight, values):
    return jnp.dot(weight, values, preferred_element_type=jnp.float32)


def kernel(
    counts, x, out, own, far_days, after, before, packed, anomaly,
    edge_own, edge_before, edge_after, edge_pass, edge_pack,
    own_sem, far_send, far_recv, near_send, near_recv, lon_send, lon_recv,
    jump_send, jump_recv, near_ready, far_ready, lon_ready,
):
    lons, days, cols = x.shape
    half = LON_HALF
    day_count, lon_count = counts
    day, lon = lax.axis_index("day"), lax.axis_index("lon")
    day_next = lax.rem(day + 1, day_count)
    day_back = lax.rem(day + day_count - 1, day_count)
    lon_next = lax.rem(lon + 1, lon_count)
    lon_back = lax.rem(lon + lon_count - 1, lon_count)
    even = lax.rem(day, 2) == 0
    odd = jnp.logical_not(even)
    far = jnp.where(even, day_back, day_next)
    near = jnp.where(even, day_next, day_back)
    low_jump = lax.rem(lon, RUN) == 0
    high_jump = lax.rem(lon, RUN) == RUN - 1
    jump = jnp.logical_or(low_jump, high_jump)
    peer = jnp.where(high_jump, lon_next, lon_back)
    edges, middle = plan(lons)
    order = edges + middle
    blocks = lons // BLOCK

    def load(b):
        rows = pl.ds(b * BLOCK, BLOCK)
        return pltpu.make_async_copy(x.at[rows], own.at[rows], own_sem.at[b])

    sequence = [0, blocks - 1, 1, blocks - 2, *range(2, blocks - 2)]
    for b in sequence:
        load(b).start()

    barrier = pltpu.get_barrier_semaphore()
    seat = lax.rem(day, 4)
    hub = seat == 1
    rest = jnp.logical_not(hub)

    def tell(semaphore, axis, *peers):
        for who in peers:
            pl.semaphore_signal(
                semaphore, inc=1, device_id={axis: who}, device_id_type=MESH
            )

    @pl.when(jnp.logical_or(hub, seat == 3))
    def _():
        tell(barrier, "day", day_back, day_next)

    @pl.when(seat == 0)
    def _():
        tell(barrier, "day", day_back)

    @pl.when(seat == 2)
    def _():
        tell(barrier, "day", day_next)

    @pl.when(rest)
    def _():
        pl.semaphore_wait(barrier, 2)

    @pl.when(seat == 0)
    def _():
        tell(near_ready, "day", day_next)

    @pl.when(seat == 2)
    def _():
        tell(far_ready, "day", day_back)

    @pl.when(hub)
    def _():
        pl.semaphore_wait(far_ready, 1)

    def remote(src, dst, send, recv, to):
        return pltpu.make_async_remote_copy(
            src_ref=src, dst_ref=dst, send_sem=send, recv_sem=recv,
            device_id=to, device_id_type=MESH,
        )

    start = pl.multiple_of(jnp.where(even, 0, ROWS), ROWS)

    def whole(n):
        at, size, _ = order[n]
        rows = pl.ds(at, size)
        return remote(
            x.at[rows, pl.ds(start, ROWS)], far_days.at[rows, pl.ds(0, ROWS)],
            far_send.at[0, n], far_recv.at[0, n], {"day": far},
        )

    def second(n):
        rows = pl.ds(*hosts(order[n]))
        return remote(
            packed.at[rows], far_days.at[rows, pl.ds(ROWS, ROWS)],
            far_send.at[1, n], far_recv.at[1, n], {"day": far},
        )

    def near_even(b):
        rows = pl.ds(b * BLOCK, BLOCK)
        return remote(
            x.at[rows, pl.ds(ROWS, DAY_HALF)], before.at[rows],
            near_send.at[b], near_recv.at[b], {"day": near},
        )

    def near_odd(b):
        rows = pl.ds(b * BLOCK, BLOCK)
        return remote(
            x.at[rows, pl.ds(0, 2 * ROWS)], after.at[rows],
            near_send.at[b], near_recv.at[b], {"day": near},
        )

    edge = pl.ds(jnp.where(high_jump, lons - half, 0), half)
    across = {"lon": peer}
    corner = {"day": far, "lon": peer}

    def jump_even():
        return remote(edge_pack, edge_own.at[:, pl.ds(2 * ROWS, ROWS)],
                      jump_send.at[0], jump_recv.at[0], across)

    def jump_odd():
        return remote(x.at[edge, pl.ds(0, ROWS)], edge_own.at[:, pl.ds(0, ROWS)],
                      jump_send.at[0], jump_recv.at[0], across)

    def corner_even():
        return [
            remote(x.at[edge, pl.ds(0, 2 * ROWS)], edge_after,
                   jump_send.at[2], jump_recv.at[2], corner),
            remote(far_days.at[edge], edge_own.at[:, pl.ds(ROWS, 2 * ROWS)],
                   jump_send.at[3], jump_recv.at[3], corner),
        ]

    def corner_odd():
        return [
            remote(x.at[edge, pl.ds(ROWS, DAY_HALF)], edge_before,
                   jump_send.at[4], jump_recv.at[4], corner),
            remote(far_days.at[edge], edge_own.at[:, pl.ds(0, 2 * ROWS)],
                   jump_send.at[5], jump_recv.at[5], corner),
        ]

    def pass_even():
        return remote(edge_own.at[:, pl.ds(ROWS, 2 * ROWS)], edge_pass,
                      jump_send.at[6], jump_recv.at[6], {"day": near})

    def pass_odd():
        return remote(edge_own.at[:, pl.ds(0, 2 * ROWS)], edge_after,
                      jump_send.at[7], jump_recv.at[7], {"day": near})

    jump_is_even = jnp.logical_and(jump, even)
    jump_is_odd = jnp.logical_and(jump, odd)

    for n in range(len(edges)):
        whole(n).start()

    @pl.when(hub)
    def _():
        pl.semaphore_wait(near_ready, 1)
        tell(barrier, "lon", lon_back, lon_next)

    @pl.when(even)
    def _():
        for b in range(blocks):
            near_even(b).start()

    @pl.when(odd)
    def _():
        for b in range(blocks):
            near_odd(b).start()

    place, col = grid(ROWS, days)
    part = DAY_HALF - ROWS
    first = jnp.where(even, ROWS, 2 * ROWS)
    keep = ones((place < part) & (col == first + place))

    def pack(n):
        at, size = hosts(order[n])
        rider = order[n][2]
        for i in range(size):
            tile = dot(keep, own[at + i])
            if rider is not None:
                ride = ones((place == part) & (col == first + i))
                tile = tile + dot(ride, own[rider])
            packed[at + i] = tile.astype(jnp.bfloat16)

    waited = 0
    for n in range(len(order)):
        at, size, _ = order[n]
        need = 2 if n < 2 else 4 if n < 4 else min(
            blocks, max(4, sequence.index(min((at + size - 1) // BLOCK, blocks - 3)) + 1)
        )
        while waited < need:
            load(sequence[waited]).wait()
            waited += 1
        if n >= len(edges):
            whole(n).start()
        pack(n)
        if n > 0:
            second(n - 1).start()
    while waited < blocks:
        load(sequence[waited]).wait()
        waited += 1
    own_band = band(3 * ROWS, days, 0)
    before_band = band(3 * ROWS, DAY_HALF, -DAY_HALF)
    after_band = band(3 * ROWS, 2 * ROWS, days)
    second(len(order) - 1).start()

    @pl.when(jump_is_even)
    def _():
        take = ones(col == DAY_HALF + place)
        for i in range(half):
            edge_pack[i] = dot(take, own[edge.start + i]).astype(jnp.bfloat16)

    @pl.when(even)
    def _():
        @pl.loop(0, blocks)
        def _(b):
            near_odd(b).wait_recv()
            for i in range(BLOCK):
                l = b * BLOCK + i
                anomaly[l + half] = dot(own_band, own[l]) + dot(after_band, after[l])

    @pl.when(odd)
    def _():
        @pl.loop(0, blocks)
        def _(b):
            near_even(b).wait_recv()
            for i in range(BLOCK):
                l = b * BLOCK + i
                anomaly[l + half] = dot(own_band, own[l]) + dot(before_band, before[l])

    @pl.when(hub)
    def _():
        pl.semaphore_wait(barrier, 2)
        tell(lon_ready, "day", day_back, day_next)

    @pl.when(seat == 0)
    def _():
        pl.semaphore_wait(lon_ready, 1)
        tell(lon_ready, "day", day_back)

    @pl.when(seat == 2)
    def _():
        pl.semaphore_wait(lon_ready, 1)
        tell(lon_ready, "day", day_next)

    @pl.when(seat == 3)
    def _():
        pl.semaphore_wait(lon_ready, 2)

    @pl.when(jump_is_even)
    def _():
        jump_even().start()
        corner_even()[0].start()

    @pl.when(jump_is_odd)
    def _():
        jump_odd().start()
        corner_odd()[0].start()

    row, other = grid(2 * ROWS, 2 * ROWS)
    way = jnp.where(even, 1, -1)
    far_band = jnp.where(
        ((other - row) * way >= 0) & (other < DAY_HALF), -1.0, 0.0
    ).astype(jnp.bfloat16)
    touched = pl.ds(start, 2 * ROWS)
    lane, source = grid(ROWS, ROWS)

    def daily(n):
        at, size, rider = order[n]
        whole(n).wait_recv()
        second(n).wait_recv()
        if rider is not None:
            host, count = hosts(order[n])
            tile = jnp.zeros((ROWS, cols), jnp.float32)
            for i in range(count):
                take = ones((lane == i) & (source == part))
                tile = tile + dot(take, far_days[host + i, pl.ds(ROWS, ROWS)])
            far_days[rider, pl.ds(ROWS, ROWS)] = tile.astype(jnp.bfloat16)
        for l in range(at, at + size):
            anomaly[l + half, touched] += dot(far_band, far_days[l])

    pieces = [
        (0, ROWS), (lons - ROWS, ROWS), (ROWS, half - ROWS), (lons - half, half - ROWS),
    ]

    def shift(n):
        at, size = pieces[n]
        low = n % 2 == 0
        place = at + half + (lons if low else -lons)
        return remote(
            anomaly.at[pl.ds(at + half, size)], anomaly.at[pl.ds(place, size)],
            lon_send.at[n], lon_recv.at[n], {"lon": lon_back if low else lon_next},
        )

    def advance(n):
        daily(n)
        if 0 < n <= len(edges):
            stays = low_jump if (n - 1) % 2 == 0 else high_jump

            @pl.when(jnp.logical_not(stays))
            def _():
                shift(n - 1).start()

    for n in range(len(edges)):
        advance(n)

    @pl.when(jump_is_even)
    def _():
        corner_even()[1].start()

    @pl.when(jump_is_odd)
    def _():
        corner_odd()[1].start()

    def pass_on():
        @pl.when(jump_is_even)
        def _():
            jump_even().wait_recv()
            corner_odd()[1].wait_recv()
            pass_even().start()

        @pl.when(jump_is_odd)
        def _():
            jump_odd().wait_recv()
            corner_even()[1].wait_recv()
            pass_odd().start()

    def zonal_edges():
        day_of, slot = grid(3 * ROWS, 3 * ROWS)
        held = jnp.where(even & (slot > DAY_HALF), slot - 1, slot)
        spare = jnp.where(even, DAY_HALF, days)
        away = jnp.abs(day_of - held)
        edge_band = jnp.where(away <= DAY_HALF, -1.0, 0.0)
        edge_band = jnp.where(away == 0, 2.0 * DAY_HALF, edge_band)
        edge_band = jnp.where(slot == spare, 0.0, edge_band).astype(jnp.bfloat16)
        to = jnp.where(high_jump, lons + half, 0)

        @pl.when(jump_is_even)
        def _():
            corner_odd()[0].wait_recv()
            pass_odd().wait_recv()
            for i in range(half):
                anomaly[to + i] = (
                    dot(edge_band, edge_own[i])
                    + dot(before_band, edge_before[i])
                    + dot(after_band, edge_after[i])
                )

        @pl.when(jump_is_odd)
        def _():
            corner_even()[0].wait_recv()
            pass_even().wait_recv()
            day_of, slot = grid(3 * ROWS, 2 * ROWS)
            held = jnp.where(slot > part, slot - 1, slot)
            pass_band = jnp.where(
                (held >= day_of) & (slot != part), -1.0, 0.0
            ).astype(jnp.bfloat16)
            for i in range(half):
                anomaly[to + i] = (
                    dot(edge_band, edge_own[i])
                    + dot(pass_band, edge_pass[i])
                    + dot(after_band, edge_after[i])
                )

        @pl.when(jnp.logical_not(high_jump))
        def _():
            shift(0).wait_recv()
            shift(2).wait_recv()

        @pl.when(jnp.logical_not(low_jump))
        def _():
            shift(1).wait_recv()
            shift(3).wait_recv()

    scale = 1.0 / ((2 * DAY_HALF + 1) * (2 * half + 1))
    width = 2 * half + 1

    def up_to(lo, hi, total):
        def step(l, total):
            total = total + (anomaly[l + width - 1] - anomaly[l - 1])
            out[l] = (total * scale)[:days]
            return total

        return lax.fori_loop(lo, hi, step, total)

    def back(step, total):
        l = half - 1 - step
        total = total + (anomaly[l] - anomaly[l + width])
        out[l] = (total * scale)[:days]
        return total

    steps = len(order)
    total = None
    done = half
    for n in range(len(edges), steps):
        end = n == steps - 1
        if n == steps - 3:
            pass_on()
        if end:
            zonal_edges()
            lax.fori_loop(0, half, back, first_total)
        advance(n)
        ready = lons if end else order[n][0] + order[n][1] - half
        if ready <= half:
            continue
        if total is None:
            total = lax.fori_loop(
                half,
                half + width,
                lambda l, t: t + anomaly[l],
                jnp.zeros((3 * ROWS, cols), jnp.float32),
            )
            out[half] = (total * scale)[:days]
            first_total = total
            done = half + 1
        total = up_to(done, ready, total)
        done = ready

    for n in range(steps):
        whole(n).wait_send()
        second(n).wait_send()

    @pl.when(even)
    def _():
        for b in range(blocks):
            near_even(b).wait_send()

    @pl.when(odd)
    def _():
        for b in range(blocks):
            near_odd(b).wait_send()

    for n in range(len(pieces)):
        stays = low_jump if n % 2 == 0 else high_jump

        @pl.when(jnp.logical_not(stays))
        def _():
            shift(n).wait_send()

    @pl.when(jump_is_even)
    def _():
        for copy in (jump_even(), *corner_even(), pass_even()):
            copy.wait_send()

    @pl.when(jump_is_odd)
    def _():
        for copy in (jump_odd(), *corner_odd(), pass_odd()):
            copy.wait_send()


def local(counts, field):
    days, lons, cols = field.shape
    x = jnp.transpose(field, (1, 0, 2))
    edges, middle = plan(lons)
    steps = len(edges) + len(middle)
    half = LON_HALF
    y = pl.pallas_call(
        functools.partial(kernel, counts),
        out_shape=pltpu.VMEM((lons, days, cols), jnp.float32),
        in_specs=[pl.BlockSpec(memory_space=pltpu.HBM)],
        out_specs=pl.BlockSpec(memory_space=pltpu.VMEM),
        scratch_shapes=[
            pltpu.VMEM((lons, days, cols), jnp.bfloat16),
            pltpu.VMEM((lons, 2 * ROWS, cols), jnp.bfloat16),
            pltpu.VMEM((lons, 2 * ROWS, cols), jnp.bfloat16),
            pltpu.VMEM((lons, DAY_HALF, cols), jnp.bfloat16),
            pltpu.VMEM((lons, ROWS, cols), jnp.bfloat16),
            pltpu.VMEM((lons + 2 * half, 3 * ROWS, cols), jnp.float32),
            pltpu.VMEM((half, 3 * ROWS, cols), jnp.bfloat16),
            pltpu.VMEM((half, DAY_HALF, cols), jnp.bfloat16),
            pltpu.VMEM((half, 2 * ROWS, cols), jnp.bfloat16),
            pltpu.VMEM((half, 2 * ROWS, cols), jnp.bfloat16),
            pltpu.VMEM((half, ROWS, cols), jnp.bfloat16),
            pltpu.SemaphoreType.DMA((lons // BLOCK,)),
            pltpu.SemaphoreType.DMA((2, steps)),
            pltpu.SemaphoreType.DMA((2, steps)),
            pltpu.SemaphoreType.DMA((lons // BLOCK,)),
            pltpu.SemaphoreType.DMA((lons // BLOCK,)),
            pltpu.SemaphoreType.DMA((4,)),
            pltpu.SemaphoreType.DMA((4,)),
            pltpu.SemaphoreType.DMA((8,)),
            pltpu.SemaphoreType.DMA((8,)),
            pltpu.SemaphoreType.REGULAR,
            pltpu.SemaphoreType.REGULAR,
            pltpu.SemaphoreType.REGULAR,
        ],
        compiler_params=pltpu.CompilerParams(
            collective_id=0, has_side_effects=True, vmem_limit_bytes=52 * 1024 * 1024
        ),
    )(x)
    return jnp.transpose(y, (1, 0, 2))


def solution(mesh):
    return jax.shard_map(
        functools.partial(local, (mesh.shape["day"], mesh.shape["lon"])),
        mesh=mesh,
        in_specs=(P("day", "lon", None),),
        out_specs=P("day", "lon", None),
        check_vma=False,
    )
```

```python
import functools

import jax
import jax.numpy as jnp
from jax import lax
from jax.experimental import pallas as pl
from jax.experimental.pallas import tpu as pltpu
from jax.sharding import PartitionSpec as P

DAY_HALF = 15
LON_HALF = 10
ROWS = 8
RUN = 8
BLOCK = 10
SHARE = 3
MESH = pl.DeviceIdType.MESH


def plan(lons):
    edges = [
        (0, ROWS, ROWS - 1),
        (lons - ROWS, ROWS, lons - ROWS),
        (ROWS, ROWS, 2 * ROWS - 1),
        (lons - 2 * ROWS, ROWS, lons - 2 * ROWS),
    ]
    middle = []
    for at in range(2 * ROWS, lons - 2 * ROWS, ROWS):
        size = min(ROWS, lons - 2 * ROWS - at)
        middle.append((at, size, at + ROWS - 1 if size == ROWS else None))
    return edges, middle


def hosts(group):
    at, size, rider = group
    if rider is None:
        return at, size
    return (at, size - 1) if rider > at else (at + 1, size - 1)


def grid(rows, cols):
    return (
        lax.broadcasted_iota(jnp.int32, (rows, cols), 0),
        lax.broadcasted_iota(jnp.int32, (rows, cols), 1),
    )


def ones(condition):
    return jnp.where(condition, 1.0, 0.0).astype(jnp.bfloat16)


def band(days, rows, shift):
    day, other = grid(days, rows)
    away = jnp.abs(day - other - shift)
    weight = jnp.where(away <= DAY_HALF, -1.0, 0.0)
    if shift == 0:
        weight = jnp.where(away == 0, 2.0 * DAY_HALF, weight)
    return weight.astype(jnp.bfloat16)


def dot(weight, values):
    return jnp.dot(weight, values, preferred_element_type=jnp.float32)


def kernel(
    counts, x, out, own, far_days, after, before, packed, anomaly,
    edge_own, edge_before, edge_after, edge_pass, edge_pack, relay,
    own_sem, far_send, far_recv, near_send, near_recv, lon_send, lon_recv,
    jump_send, jump_recv, near_ready, far_ready, lon_ready,
    chain_ready, jump_ready,
):
    lons, days, cols = x.shape
    half = LON_HALF
    day_count, lon_count = counts
    day, lon = lax.axis_index("day"), lax.axis_index("lon")
    day_next = lax.rem(day + 1, day_count)
    day_back = lax.rem(day + day_count - 1, day_count)
    lon_next = lax.rem(lon + 1, lon_count)
    lon_back = lax.rem(lon + lon_count - 1, lon_count)
    even = lax.rem(day, 2) == 0
    odd = jnp.logical_not(even)
    far = jnp.where(even, day_back, day_next)
    near = jnp.where(even, day_next, day_back)
    zone = lax.rem(lon, RUN)
    low = zone < RUN // 2
    reach = jnp.where(low, zone, RUN - 1 - zone)
    toward = jnp.where(low, lon_back, lon_next)
    low_jump = zone == 0
    high_jump = zone == RUN - 1
    jump = jnp.logical_or(low_jump, high_jump)
    peer = jnp.where(high_jump, lon_next, lon_back)
    edges, middle = plan(lons)
    order = edges + middle
    blocks = lons // BLOCK

    def load(b):
        rows = pl.ds(b * BLOCK, BLOCK)
        return pltpu.make_async_copy(x.at[rows], own.at[rows], own_sem.at[b])

    sequence = [0, blocks - 1, 1, blocks - 2, *range(2, blocks - 2)]
    for b in sequence:
        load(b).start()

    barrier = pltpu.get_barrier_semaphore()
    seat = lax.rem(day, 4)
    hub = seat == 1
    rest = jnp.logical_not(hub)

    def tell(semaphore, axis, *peers):
        for who in peers:
            pl.semaphore_signal(
                semaphore, inc=1, device_id={axis: who}, device_id_type=MESH
            )

    @pl.when(jnp.logical_or(hub, seat == 3))
    def _():
        tell(barrier, "day", day_back, day_next)

    @pl.when(seat == 0)
    def _():
        tell(barrier, "day", day_back)

    @pl.when(seat == 2)
    def _():
        tell(barrier, "day", day_next)

    @pl.when(rest)
    def _():
        pl.semaphore_wait(barrier, 2)

    @pl.when(seat == 0)
    def _():
        tell(near_ready, "day", day_next)

    @pl.when(seat == 2)
    def _():
        tell(far_ready, "day", day_back)

    @pl.when(hub)
    def _():
        pl.semaphore_wait(far_ready, 1)

    def remote(src, dst, send, recv, to):
        return pltpu.make_async_remote_copy(
            src_ref=src, dst_ref=dst, send_sem=send, recv_sem=recv,
            device_id=to, device_id_type=MESH,
        )

    start = pl.multiple_of(jnp.where(even, 0, ROWS), ROWS)

    def whole(n):
        at, size, _ = order[n]
        rows = pl.ds(at, size)
        return remote(
            x.at[rows, pl.ds(start, ROWS)], far_days.at[rows, pl.ds(0, ROWS)],
            far_send.at[0, n], far_recv.at[0, n], {"day": far},
        )

    def second(n):
        rows = pl.ds(*hosts(order[n]))
        return remote(
            packed.at[rows], far_days.at[rows, pl.ds(ROWS, ROWS)],
            far_send.at[1, n], far_recv.at[1, n], {"day": far},
        )

    def near_even(b):
        rows = pl.ds(b * BLOCK, BLOCK)
        return remote(
            x.at[rows, pl.ds(ROWS, DAY_HALF)], before.at[rows],
            near_send.at[b], near_recv.at[b], {"day": near},
        )

    def near_odd(b):
        rows = pl.ds(b * BLOCK, BLOCK)
        return remote(
            x.at[rows, pl.ds(0, 2 * ROWS)], after.at[rows],
            near_send.at[b], near_recv.at[b], {"day": near},
        )

    edge = pl.ds(jnp.where(high_jump, lons - half, 0), half)
    across = {"lon": peer}
    corner = {"day": far, "lon": peer}

    row_of = pl.multiple_of(jnp.where(even, 2 * ROWS, 0), ROWS)
    relays = RUN // 2 - 1
    direct = half - relays * SHARE

    def jump_direct():
        rows = pl.ds(0, direct)
        return remote(edge_pack.at[rows], edge_own.at[rows, pl.ds(row_of, ROWS)],
                      jump_send.at[0], jump_recv.at[0], across)

    def jump_relay(r):
        by = lax.rem(jnp.where(high_jump, lon + 1 + r, lon + lon_count - 1 - r), lon_count)
        return remote(edge_pack.at[pl.ds(direct + (r - 1) * SHARE, SHARE)], relay,
                      jump_send.at[7 + r], jump_recv.at[1], {"lon": by})

    def relay_out(r):
        rows = pl.ds(direct + (r - 1) * SHARE, SHARE)
        return remote(relay, edge_own.at[rows, pl.ds(row_of, ROWS)],
                      jump_send.at[1], jump_recv.at[7 + r],
                      {"lon": jnp.where(low, lon - reach, lon + reach)})

    def corner_even():
        return [
            remote(x.at[edge, pl.ds(0, 2 * ROWS)], edge_after,
                   jump_send.at[2], jump_recv.at[2], corner),
            remote(far_days.at[edge], edge_own.at[:, pl.ds(ROWS, 2 * ROWS)],
                   jump_send.at[3], jump_recv.at[3], corner),
        ]

    def corner_odd():
        return [
            remote(x.at[edge, pl.ds(ROWS, DAY_HALF)], edge_before,
                   jump_send.at[4], jump_recv.at[4], corner),
            remote(far_days.at[edge], edge_own.at[:, pl.ds(0, 2 * ROWS)],
                   jump_send.at[5], jump_recv.at[5], corner),
        ]

    def pass_even():
        return remote(edge_own.at[:, pl.ds(ROWS, 2 * ROWS)], edge_pass,
                      jump_send.at[6], jump_recv.at[6], {"day": near})

    def pass_odd():
        return remote(edge_own.at[:, pl.ds(0, 2 * ROWS)], edge_after,
                      jump_send.at[7], jump_recv.at[7], {"day": near})

    jump_is_even = jnp.logical_and(jump, even)
    jump_is_odd = jnp.logical_and(jump, odd)

    for n in range(len(edges)):
        whole(n).start()

    @pl.when(hub)
    def _():
        pl.semaphore_wait(near_ready, 1)
        tell(barrier, "lon", lon_back, lon_next)

    @pl.when(even)
    def _():
        for b in range(blocks):
            near_even(b).start()

    @pl.when(odd)
    def _():
        for b in range(blocks):
            near_odd(b).start()

    place, col = grid(ROWS, days)
    part = DAY_HALF - ROWS
    first = jnp.where(even, ROWS, 2 * ROWS)
    keep = ones((place < part) & (col == first + place))

    def pack(n):
        at, size = hosts(order[n])
        rider = order[n][2]
        for i in range(size):
            tile = dot(keep, own[at + i])
            if rider is not None:
                ride = ones((place == part) & (col == first + i))
                tile = tile + dot(ride, own[rider])
            packed[at + i] = tile.astype(jnp.bfloat16)

    waited = 0
    for n in range(len(order)):
        at, size, _ = order[n]
        need = 2 if n < 2 else 4 if n < 4 else min(
            blocks, max(4, sequence.index(min((at + size - 1) // BLOCK, blocks - 3)) + 1)
        )
        while waited < need:
            load(sequence[waited]).wait()
            waited += 1
        if n >= len(edges):
            whole(n).start()
        pack(n)
        if n > 0:
            second(n - 1).start()
    while waited < blocks:
        load(sequence[waited]).wait()
        waited += 1
    own_band = band(3 * ROWS, days, 0)
    before_band = band(3 * ROWS, DAY_HALF, -DAY_HALF)
    after_band = band(3 * ROWS, 2 * ROWS, days)
    second(len(order) - 1).start()

    @pl.when(jump)
    def _():
        take = ones(col == jnp.where(even, DAY_HALF, 0) + place)
        for i in range(half):
            edge_pack[i] = dot(take, own[edge.start + i]).astype(jnp.bfloat16)

    @pl.when(even)
    def _():
        @pl.loop(0, blocks)
        def _(b):
            near_odd(b).wait_recv()
            for i in range(BLOCK):
                l = b * BLOCK + i
                anomaly[l + half] = dot(own_band, own[l]) + dot(after_band, after[l])

    @pl.when(odd)
    def _():
        @pl.loop(0, blocks)
        def _(b):
            near_even(b).wait_recv()
            for i in range(BLOCK):
                l = b * BLOCK + i
                anomaly[l + half] = dot(own_band, own[l]) + dot(before_band, before[l])

    @pl.when(hub)
    def _():
        pl.semaphore_wait(barrier, 2)
        tell(lon_ready, "day", day_back, day_next)

    @pl.when(seat == 0)
    def _():
        pl.semaphore_wait(lon_ready, 1)
        tell(lon_ready, "day", day_back)

    @pl.when(seat == 2)
    def _():
        pl.semaphore_wait(lon_ready, 1)
        tell(lon_ready, "day", day_next)

    @pl.when(seat == 3)
    def _():
        pl.semaphore_wait(lon_ready, 2)

    @pl.when(jump_is_even)
    def _():
        corner_even()[0].start()

    @pl.when(jump_is_odd)
    def _():
        corner_odd()[0].start()

    @pl.when(reach == 2)
    def _():
        tell(chain_ready, "lon", toward)

    @pl.when(reach == 1)
    def _():
        pl.semaphore_wait(chain_ready, 1)
        tell(chain_ready, "lon", toward)

    @pl.when(jump)
    def _():
        pl.semaphore_wait(chain_ready, 1)
        tell(jump_ready, "lon", toward)
        pl.semaphore_wait(jump_ready, 1)
        jump_direct().start()
        for r in range(1, relays + 1):
            jump_relay(r).start()

    row, other = grid(2 * ROWS, 2 * ROWS)
    way = jnp.where(even, 1, -1)
    far_band = jnp.where(
        ((other - row) * way >= 0) & (other < DAY_HALF), -1.0, 0.0
    ).astype(jnp.bfloat16)
    touched = pl.ds(start, 2 * ROWS)
    lane, source = grid(ROWS, ROWS)

    def daily(n):
        at, size, rider = order[n]
        whole(n).wait_recv()
        second(n).wait_recv()
        if rider is not None:
            host, count = hosts(order[n])
            tile = jnp.zeros((ROWS, cols), jnp.float32)
            for i in range(count):
                take = ones((lane == i) & (source == part))
                tile = tile + dot(take, far_days[host + i, pl.ds(ROWS, ROWS)])
            far_days[rider, pl.ds(ROWS, ROWS)] = tile.astype(jnp.bfloat16)
        for l in range(at, at + size):
            anomaly[l + half, touched] += dot(far_band, far_days[l])

    pieces = [
        (0, ROWS), (lons - ROWS, ROWS), (ROWS, half - ROWS), (lons - half, half - ROWS),
    ]

    def shift(n):
        at, size = pieces[n]
        down = n % 2 == 0
        place = at + half + (lons if down else -lons)
        return remote(
            anomaly.at[pl.ds(at + half, size)], anomaly.at[pl.ds(place, size)],
            lon_send.at[n], lon_recv.at[n], {"lon": lon_back if down else lon_next},
        )

    def advance(n):
        daily(n)
        if 0 < n <= len(edges):
            stays = low_jump if (n - 1) % 2 == 0 else high_jump

            @pl.when(jnp.logical_not(stays))
            def _():
                shift(n - 1).start()

    for n in range(len(edges)):
        advance(n)

    @pl.when(jump_is_even)
    def _():
        corner_even()[1].start()

    @pl.when(jump_is_odd)
    def _():
        corner_odd()[1].start()

    def pass_on():
        @pl.when(jump)
        def _():
            jump_direct().wait_recv()
            for r in range(1, relays + 1):
                relay_out(r).wait_recv()

        @pl.when(jump_is_even)
        def _():
            corner_odd()[1].wait_recv()
            pass_even().start()

        @pl.when(jump_is_odd)
        def _():
            corner_even()[1].wait_recv()
            pass_odd().start()

    def zonal_edges():
        day_of, slot = grid(3 * ROWS, 3 * ROWS)
        held = jnp.where(even & (slot > DAY_HALF), slot - 1, slot)
        spare = jnp.where(even, DAY_HALF, days)
        away = jnp.abs(day_of - held)
        edge_band = jnp.where(away <= DAY_HALF, -1.0, 0.0)
        edge_band = jnp.where(away == 0, 2.0 * DAY_HALF, edge_band)
        edge_band = jnp.where(slot == spare, 0.0, edge_band).astype(jnp.bfloat16)
        to = jnp.where(high_jump, lons + half, 0)

        @pl.when(jump_is_even)
        def _():
            corner_odd()[0].wait_recv()
            pass_odd().wait_recv()
            for i in range(half):
                anomaly[to + i] = (
                    dot(edge_band, edge_own[i])
                    + dot(before_band, edge_before[i])
                    + dot(after_band, edge_after[i])
                )

        @pl.when(jump_is_odd)
        def _():
            corner_even()[0].wait_recv()
            pass_even().wait_recv()
            day_of, slot = grid(3 * ROWS, 2 * ROWS)
            held = jnp.where(slot > part, slot - 1, slot)
            pass_band = jnp.where(
                (held >= day_of) & (slot != part), -1.0, 0.0
            ).astype(jnp.bfloat16)
            for i in range(half):
                anomaly[to + i] = (
                    dot(edge_band, edge_own[i])
                    + dot(pass_band, edge_pass[i])
                    + dot(after_band, edge_after[i])
                )

        @pl.when(jnp.logical_not(high_jump))
        def _():
            shift(0).wait_recv()
            shift(2).wait_recv()

        @pl.when(jnp.logical_not(low_jump))
        def _():
            shift(1).wait_recv()
            shift(3).wait_recv()

    scale = 1.0 / ((2 * DAY_HALF + 1) * (2 * half + 1))
    width = 2 * half + 1

    def up_to(lo, hi, total):
        def step(l, total):
            total = total + (anomaly[l + width - 1] - anomaly[l - 1])
            out[l] = (total * scale)[:days]
            return total

        return lax.fori_loop(lo, hi, step, total)

    def back(step, total):
        l = half - 1 - step
        total = total + (anomaly[l] - anomaly[l + width])
        out[l] = (total * scale)[:days]
        return total

    steps = len(order)
    total = None
    done = half
    for n in range(len(edges), steps):
        end = n == steps - 1
        if n == steps - 5:
            @pl.when(reach > 0)
            def _():
                jump_relay(1).wait_recv()
                relay_out(reach).start()
        if n == steps - 4:
            pass_on()
        if n == steps - 2:
            zonal_edges()
            lax.fori_loop(0, half, back, first_total)
        advance(n)
        ready = lons if end else order[n][0] + order[n][1] - half
        if ready <= half:
            continue
        if total is None:
            total = lax.fori_loop(
                half,
                half + width,
                lambda l, t: t + anomaly[l],
                jnp.zeros((3 * ROWS, cols), jnp.float32),
            )
            out[half] = (total * scale)[:days]
            first_total = total
            done = half + 1
        total = up_to(done, ready, total)
        done = ready

    for n in range(steps):
        whole(n).wait_send()
        second(n).wait_send()

    @pl.when(even)
    def _():
        for b in range(blocks):
            near_even(b).wait_send()

    @pl.when(odd)
    def _():
        for b in range(blocks):
            near_odd(b).wait_send()

    for n in range(len(pieces)):
        stays = low_jump if n % 2 == 0 else high_jump

        @pl.when(jnp.logical_not(stays))
        def _():
            shift(n).wait_send()

    @pl.when(jump)
    def _():
        jump_direct().wait_send()
        for r in range(1, relays + 1):
            jump_relay(r).wait_send()

    @pl.when(reach > 0)
    def _():
        relay_out(reach).wait_send()

    @pl.when(jump_is_even)
    def _():
        for copy in (*corner_even(), pass_even()):
            copy.wait_send()

    @pl.when(jump_is_odd)
    def _():
        for copy in (*corner_odd(), pass_odd()):
            copy.wait_send()


def local(counts, field):
    days, lons, cols = field.shape
    x = jnp.transpose(field, (1, 0, 2))
    edges, middle = plan(lons)
    steps = len(edges) + len(middle)
    half = LON_HALF
    y = pl.pallas_call(
        functools.partial(kernel, counts),
        out_shape=pltpu.VMEM((lons, days, cols), jnp.float32),
        in_specs=[pl.BlockSpec(memory_space=pltpu.HBM)],
        out_specs=pl.BlockSpec(memory_space=pltpu.VMEM),
        scratch_shapes=[
            pltpu.VMEM((lons, days, cols), jnp.bfloat16),
            pltpu.VMEM((lons, 2 * ROWS, cols), jnp.bfloat16),
            pltpu.VMEM((lons, 2 * ROWS, cols), jnp.bfloat16),
            pltpu.VMEM((lons, DAY_HALF, cols), jnp.bfloat16),
            pltpu.VMEM((lons, ROWS, cols), jnp.bfloat16),
            pltpu.VMEM((lons + 2 * half, 3 * ROWS, cols), jnp.float32),
            pltpu.VMEM((half, 3 * ROWS, cols), jnp.bfloat16),
            pltpu.VMEM((half, DAY_HALF, cols), jnp.bfloat16),
            pltpu.VMEM((half, 2 * ROWS, cols), jnp.bfloat16),
            pltpu.VMEM((half, 2 * ROWS, cols), jnp.bfloat16),
            pltpu.VMEM((half, ROWS, cols), jnp.bfloat16),
            pltpu.VMEM((SHARE, ROWS, cols), jnp.bfloat16),
            pltpu.SemaphoreType.DMA((lons // BLOCK,)),
            pltpu.SemaphoreType.DMA((2, steps)),
            pltpu.SemaphoreType.DMA((2, steps)),
            pltpu.SemaphoreType.DMA((lons // BLOCK,)),
            pltpu.SemaphoreType.DMA((lons // BLOCK,)),
            pltpu.SemaphoreType.DMA((4,)),
            pltpu.SemaphoreType.DMA((4,)),
            pltpu.SemaphoreType.DMA((11,)),
            pltpu.SemaphoreType.DMA((11,)),
            pltpu.SemaphoreType.REGULAR,
            pltpu.SemaphoreType.REGULAR,
            pltpu.SemaphoreType.REGULAR,
            pltpu.SemaphoreType.REGULAR,
            pltpu.SemaphoreType.REGULAR,
        ],
        compiler_params=pltpu.CompilerParams(
            collective_id=0, has_side_effects=True, vmem_limit_bytes=52 * 1024 * 1024
        ),
    )(x)
    return jnp.transpose(y, (1, 0, 2))


def solution(mesh):
    return jax.shard_map(
        functools.partial(local, (mesh.shape["day"], mesh.shape["lon"])),
        mesh=mesh,
        in_specs=(P("day", "lon", None),),
        out_specs=P("day", "lon", None),
        check_vma=False,
    )
```

```python
import functools

import jax
import jax.numpy as jnp
from jax import lax
from jax.experimental import pallas as pl
from jax.experimental.pallas import tpu as pltpu
from jax.sharding import PartitionSpec as P

DAY_HALF = 15
LON_HALF = 10
ROWS = 8
RUN = 8
BLOCK = 10
SHARE = 3
MESH = pl.DeviceIdType.MESH


def plan(lons):
    edges = [
        (0, ROWS, ROWS - 1),
        (lons - ROWS, ROWS, lons - ROWS),
        (ROWS, ROWS, 2 * ROWS - 1),
        (lons - 2 * ROWS, ROWS, lons - 2 * ROWS),
    ]
    middle = []
    for at in range(2 * ROWS, lons - 2 * ROWS, ROWS):
        size = min(ROWS, lons - 2 * ROWS - at)
        middle.append((at, size, at + ROWS - 1 if size == ROWS else None))
    return edges, middle


def hosts(group):
    at, size, rider = group
    if rider is None:
        return at, size
    return (at, size - 1) if rider > at else (at + 1, size - 1)


def grid(rows, cols):
    return (
        lax.broadcasted_iota(jnp.int32, (rows, cols), 0),
        lax.broadcasted_iota(jnp.int32, (rows, cols), 1),
    )


def ones(condition):
    return jnp.where(condition, 1.0, 0.0).astype(jnp.bfloat16)


def band(days, rows, shift):
    day, other = grid(days, rows)
    away = jnp.abs(day - other - shift)
    weight = jnp.where(away <= DAY_HALF, -1.0, 0.0)
    if shift == 0:
        weight = jnp.where(away == 0, 2.0 * DAY_HALF, weight)
    return weight.astype(jnp.bfloat16)


def dot(weight, values):
    return jnp.dot(weight, values, preferred_element_type=jnp.float32)


def kernel(
    counts, x, out, anomaly, own, far_days, after, before, packed,
    edge_own, edge_before, edge_after, edge_pass, edge_pack, relay,
    own_sem, far_send, far_recv, near_send, near_recv, lon_send, lon_recv,
    jump_send, jump_recv, near_ready, far_ready, lon_ready,
    chain_ready, jump_ready,
):
    lons, days, cols = x.shape
    half = LON_HALF
    day_count, lon_count = counts
    day, lon = lax.axis_index("day"), lax.axis_index("lon")
    day_next = lax.rem(day + 1, day_count)
    day_back = lax.rem(day + day_count - 1, day_count)
    lon_next = lax.rem(lon + 1, lon_count)
    lon_back = lax.rem(lon + lon_count - 1, lon_count)
    even = lax.rem(day, 2) == 0
    odd = jnp.logical_not(even)
    far = jnp.where(even, day_back, day_next)
    near = jnp.where(even, day_next, day_back)
    zone = lax.rem(lon, RUN)
    low = zone < RUN // 2
    reach = jnp.where(low, zone, RUN - 1 - zone)
    toward = jnp.where(low, lon_back, lon_next)
    low_jump = zone == 0
    high_jump = zone == RUN - 1
    jump = jnp.logical_or(low_jump, high_jump)
    peer = jnp.where(high_jump, lon_next, lon_back)
    edges, middle = plan(lons)
    order = edges + middle
    blocks = lons // BLOCK

    def load(b):
        rows = pl.ds(b * BLOCK, BLOCK)
        return pltpu.make_async_copy(x.at[rows], own.at[rows], own_sem.at[b])

    sequence = [0, blocks - 1, 1, blocks - 2, *range(2, blocks - 2)]
    for b in sequence:
        load(b).start()

    barrier = pltpu.get_barrier_semaphore()
    seat = lax.rem(day, 4)
    hub = seat == 0
    rest = jnp.logical_not(hub)

    def tell(semaphore, axis, *peers):
        for who in peers:
            pl.semaphore_signal(
                semaphore, inc=1, device_id={axis: who}, device_id_type=MESH
            )

    @pl.when(jnp.logical_or(hub, seat == 2))
    def _():
        tell(barrier, "day", day_back, day_next)

    @pl.when(seat == 1)
    def _():
        tell(barrier, "day", day_next)

    @pl.when(seat == 3)
    def _():
        tell(barrier, "day", day_back)

    @pl.when(rest)
    def _():
        pl.semaphore_wait(barrier, 2)

    @pl.when(seat == 1)
    def _():
        tell(near_ready, "day", day_back)

    @pl.when(seat == 3)
    def _():
        tell(far_ready, "day", day_next)

    @pl.when(hub)
    def _():
        pl.semaphore_wait(far_ready, 1)

    def remote(src, dst, send, recv, to):
        return pltpu.make_async_remote_copy(
            src_ref=src, dst_ref=dst, send_sem=send, recv_sem=recv,
            device_id=to, device_id_type=MESH,
        )

    start = pl.multiple_of(jnp.where(even, 0, ROWS), ROWS)

    def whole(n):
        at, size, _ = order[n]
        rows = pl.ds(at, size)
        return remote(
            (own if n else x).at[rows, pl.ds(start, ROWS)], far_days.at[rows, pl.ds(0, ROWS)],
            far_send.at[0, n], far_recv.at[0, n], {"day": far},
        )

    def second(n):
        rows = pl.ds(*hosts(order[n]))
        return remote(
            packed.at[rows], far_days.at[rows, pl.ds(ROWS, ROWS)],
            far_send.at[1, n], far_recv.at[1, n], {"day": far},
        )

    def near_even(b):
        rows = pl.ds(b * BLOCK, BLOCK)
        return remote(
            x.at[rows, pl.ds(ROWS, DAY_HALF)], before.at[rows],
            near_send.at[b], near_recv.at[b], {"day": near},
        )

    def near_odd(b):
        rows = pl.ds(b * BLOCK, BLOCK)
        return remote(
            x.at[rows, pl.ds(0, 2 * ROWS)], after.at[rows],
            near_send.at[b], near_recv.at[b], {"day": near},
        )

    edge = pl.ds(jnp.where(high_jump, lons - half, 0), half)
    across = {"lon": peer}
    corner = {"day": far, "lon": peer}

    row_of = pl.multiple_of(jnp.where(even, 2 * ROWS, 0), ROWS)
    relays = RUN // 2 - 1
    direct = half - relays * SHARE

    def jump_direct():
        rows = pl.ds(0, direct)
        return remote(edge_pack.at[rows], edge_own.at[rows, pl.ds(row_of, ROWS)],
                      jump_send.at[0], jump_recv.at[0], across)

    def jump_relay(r):
        by = lax.rem(jnp.where(high_jump, lon + 1 + r, lon + lon_count - 1 - r), lon_count)
        return remote(edge_pack.at[pl.ds(direct + (r - 1) * SHARE, SHARE)], relay,
                      jump_send.at[7 + r], jump_recv.at[1], {"lon": by})

    def relay_out(r):
        rows = pl.ds(direct + (r - 1) * SHARE, SHARE)
        return remote(relay, edge_own.at[rows, pl.ds(row_of, ROWS)],
                      jump_send.at[1], jump_recv.at[7 + r],
                      {"lon": jnp.where(low, lon - reach, lon + reach)})

    def corner_even():
        return [
            remote(x.at[edge, pl.ds(0, 2 * ROWS)], edge_after,
                   jump_send.at[2], jump_recv.at[2], corner),
            remote(far_days.at[edge], edge_own.at[:, pl.ds(ROWS, 2 * ROWS)],
                   jump_send.at[3], jump_recv.at[3], corner),
        ]

    def corner_odd():
        return [
            remote(x.at[edge, pl.ds(ROWS, DAY_HALF)], edge_before,
                   jump_send.at[4], jump_recv.at[4], corner),
            remote(far_days.at[edge], edge_own.at[:, pl.ds(0, 2 * ROWS)],
                   jump_send.at[5], jump_recv.at[5], corner),
        ]

    def pass_even():
        return remote(edge_own.at[:, pl.ds(ROWS, 2 * ROWS)], edge_pass,
                      jump_send.at[6], jump_recv.at[6], {"day": near})

    def pass_odd():
        return remote(edge_own.at[:, pl.ds(0, 2 * ROWS)], edge_after,
                      jump_send.at[7], jump_recv.at[7], {"day": near})

    jump_is_even = jnp.logical_and(jump, even)
    jump_is_odd = jnp.logical_and(jump, odd)

    waited = [0]

    def loaded(count):
        while waited[0] < count:
            load(sequence[waited[0]]).wait()
            waited[0] += 1

    for n in range(len(edges)):
        if n:
            loaded(n + 1)
        whole(n).start()

    @pl.when(hub)
    def _():
        pl.semaphore_wait(near_ready, 1)
        tell(barrier, "lon", lon_back, lon_next)

    @pl.when(even)
    def _():
        for b in range(blocks):
            near_even(b).start()

    @pl.when(odd)
    def _():
        for b in range(blocks):
            near_odd(b).start()

    place, col = grid(ROWS, days)
    part = DAY_HALF - ROWS
    first = jnp.where(even, ROWS, 2 * ROWS)
    keep = ones((place < part) & (col == first + place))

    def pack(n):
        at, size = hosts(order[n])
        rider = order[n][2]
        for i in range(size):
            tile = dot(keep, own[at + i])
            if rider is not None:
                ride = ones((place == part) & (col == first + i))
                tile = tile + dot(ride, own[rider])
            packed[at + i] = tile.astype(jnp.bfloat16)

    for n in range(len(order)):
        at, size, _ = order[n]
        if n >= len(edges):
            last = min((at + size - 1) // BLOCK, blocks - 3)
            loaded(max(4, sequence.index(last) + 1))
        if n >= len(edges):
            whole(n).start()
        pack(n)
        if n > 0:
            second(n - 1).start()
    loaded(blocks)
    own_band = band(3 * ROWS, days, 0)
    before_band = band(3 * ROWS, DAY_HALF, -DAY_HALF)
    after_band = band(3 * ROWS, 2 * ROWS, days)
    second(len(order) - 1).start()

    @pl.when(jump)
    def _():
        take = ones(col == jnp.where(even, DAY_HALF, 0) + place)
        for i in range(half):
            edge_pack[i] = dot(take, own[edge.start + i]).astype(jnp.bfloat16)

    @pl.when(even)
    def _():
        @pl.loop(0, blocks)
        def _(b):
            near_odd(b).wait_recv()
            for i in range(BLOCK):
                l = b * BLOCK + i
                anomaly[l + half] = dot(own_band, own[l]) + dot(after_band, after[l])

    @pl.when(odd)
    def _():
        @pl.loop(0, blocks)
        def _(b):
            near_even(b).wait_recv()
            for i in range(BLOCK):
                l = b * BLOCK + i
                anomaly[l + half] = dot(own_band, own[l]) + dot(before_band, before[l])

    @pl.when(hub)
    def _():
        pl.semaphore_wait(barrier, 2)
        tell(lon_ready, "day", day_back, day_next)

    @pl.when(seat == 1)
    def _():
        pl.semaphore_wait(lon_ready, 1)
        tell(lon_ready, "day", day_next)

    @pl.when(seat == 3)
    def _():
        pl.semaphore_wait(lon_ready, 1)
        tell(lon_ready, "day", day_back)

    @pl.when(seat == 2)
    def _():
        pl.semaphore_wait(lon_ready, 2)

    @pl.when(jump_is_even)
    def _():
        corner_even()[0].start()

    @pl.when(jump_is_odd)
    def _():
        corner_odd()[0].start()

    @pl.when(reach == 2)
    def _():
        tell(chain_ready, "lon", toward)

    @pl.when(reach == 1)
    def _():
        pl.semaphore_wait(chain_ready, 1)
        tell(chain_ready, "lon", toward)

    @pl.when(jump)
    def _():
        pl.semaphore_wait(chain_ready, 1)
        tell(jump_ready, "lon", toward)
        pl.semaphore_wait(jump_ready, 1)
        jump_direct().start()
        for r in range(1, relays + 1):
            jump_relay(r).start()

    row, other = grid(2 * ROWS, 2 * ROWS)
    way = jnp.where(even, 1, -1)
    far_band = jnp.where(
        ((other - row) * way >= 0) & (other < DAY_HALF), -1.0, 0.0
    ).astype(jnp.bfloat16)
    touched = pl.ds(start, 2 * ROWS)
    lane, source = grid(ROWS, ROWS)

    def daily(n):
        at, size, rider = order[n]
        whole(n).wait_recv()
        second(n).wait_recv()
        if rider is not None:
            host, count = hosts(order[n])
            tile = jnp.zeros((ROWS, cols), jnp.float32)
            for i in range(count):
                take = ones((lane == i) & (source == part))
                tile = tile + dot(take, far_days[host + i, pl.ds(ROWS, ROWS)])
            far_days[rider, pl.ds(ROWS, ROWS)] = tile.astype(jnp.bfloat16)
        for l in range(at, at + size):
            anomaly[l + half, touched] += dot(far_band, far_days[l])

    pieces = [
        (0, ROWS), (lons - ROWS, ROWS), (ROWS, half - ROWS), (lons - half, half - ROWS),
    ]

    def shift(n):
        at, size = pieces[n]
        down = n % 2 == 0
        place = at + half + (lons if down else -lons)
        return remote(
            anomaly.at[pl.ds(at + half, size)], anomaly.at[pl.ds(place, size)],
            lon_send.at[n], lon_recv.at[n], {"lon": lon_back if down else lon_next},
        )

    def advance(n):
        daily(n)
        if 0 < n <= len(edges):
            stays = low_jump if (n - 1) % 2 == 0 else high_jump

            @pl.when(jnp.logical_not(stays))
            def _():
                shift(n - 1).start()

    for n in range(len(edges)):
        advance(n)

    @pl.when(jump_is_even)
    def _():
        corner_even()[1].start()

    @pl.when(jump_is_odd)
    def _():
        corner_odd()[1].start()

    def pass_on():
        @pl.when(jump)
        def _():
            jump_direct().wait_recv()
            for r in range(1, relays + 1):
                relay_out(r).wait_recv()

        @pl.when(jump_is_even)
        def _():
            corner_odd()[1].wait_recv()
            pass_even().start()

        @pl.when(jump_is_odd)
        def _():
            corner_even()[1].wait_recv()
            pass_odd().start()

    def zonal_edges():
        day_of, slot = grid(3 * ROWS, 3 * ROWS)
        held = jnp.where(even & (slot > DAY_HALF), slot - 1, slot)
        spare = jnp.where(even, DAY_HALF, days)
        away = jnp.abs(day_of - held)
        edge_band = jnp.where(away <= DAY_HALF, -1.0, 0.0)
        edge_band = jnp.where(away == 0, 2.0 * DAY_HALF, edge_band)
        edge_band = jnp.where(slot == spare, 0.0, edge_band).astype(jnp.bfloat16)
        to = jnp.where(high_jump, lons + half, 0)

        @pl.when(jump_is_even)
        def _():
            corner_odd()[0].wait_recv()
            pass_odd().wait_recv()
            for i in range(half):
                anomaly[to + i] = (
                    dot(edge_band, edge_own[i])
                    + dot(before_band, edge_before[i])
                    + dot(after_band, edge_after[i])
                )

        @pl.when(jump_is_odd)
        def _():
            corner_even()[0].wait_recv()
            pass_even().wait_recv()
            day_of, slot = grid(3 * ROWS, 2 * ROWS)
            held = jnp.where(slot > part, slot - 1, slot)
            pass_band = jnp.where(
                (held >= day_of) & (slot != part), -1.0, 0.0
            ).astype(jnp.bfloat16)
            for i in range(half):
                anomaly[to + i] = (
                    dot(edge_band, edge_own[i])
                    + dot(pass_band, edge_pass[i])
                    + dot(after_band, edge_after[i])
                )

        @pl.when(jnp.logical_not(high_jump))
        def _():
            shift(0).wait_recv()
            shift(2).wait_recv()

        @pl.when(jnp.logical_not(low_jump))
        def _():
            shift(1).wait_recv()
            shift(3).wait_recv()

    scale = 1.0 / ((2 * DAY_HALF + 1) * (2 * half + 1))
    width = 2 * half + 1

    def up_to(lo, hi, total):
        def step(l, total):
            total = total + (anomaly[l + width - 1] - anomaly[l - 1])
            out[l] = (total * scale)[:days]
            return total

        return lax.fori_loop(lo, hi, step, total)

    def back(step, total):
        l = half - 1 - step
        total = total + (anomaly[l] - anomaly[l + width])
        out[l] = (total * scale)[:days]
        return total

    steps = len(order)
    total = None
    done = half
    for n in range(len(edges), steps):
        end = n == steps - 1
        if n == steps - 5:
            @pl.when(reach > 0)
            def _():
                jump_relay(1).wait_recv()
                relay_out(reach).start()
        if n == steps - 4:
            pass_on()
        if n == steps - 2:
            zonal_edges()
            lax.fori_loop(0, half, back, first_total)
        advance(n)
        ready = order[n][0] + order[n][1] - half
        if ready <= half or end:
            continue
        if total is None:
            total = lax.fori_loop(
                half,
                half + width,
                lambda l, t: t + anomaly[l],
                jnp.zeros((3 * ROWS, cols), jnp.float32),
            )
            out[half] = (total * scale)[:days]
            first_total = total
            done = half + 1
        total = up_to(done, ready, total)
        done = ready

    for n in range(steps):
        whole(n).wait_send()
        second(n).wait_send()

    @pl.when(even)
    def _():
        for b in range(blocks):
            near_even(b).wait_send()

    @pl.when(odd)
    def _():
        for b in range(blocks):
            near_odd(b).wait_send()

    for n in range(len(pieces)):
        stays = low_jump if n % 2 == 0 else high_jump

        @pl.when(jnp.logical_not(stays))
        def _():
            shift(n).wait_send()

    @pl.when(jump)
    def _():
        jump_direct().wait_send()
        for r in range(1, relays + 1):
            jump_relay(r).wait_send()

    @pl.when(reach > 0)
    def _():
        relay_out(reach).wait_send()

    @pl.when(jump_is_even)
    def _():
        for copy in (*corner_even(), pass_even()):
            copy.wait_send()

    @pl.when(jump_is_odd)
    def _():
        for copy in (*corner_odd(), pass_odd()):
            copy.wait_send()


def store(held, anomaly, out, last, done):
    split, days, _ = held.shape
    count = last.shape[0]
    half = LON_HALF
    width = 2 * half + 1
    scale = 1.0 / ((2 * DAY_HALF + 1) * width)
    copies = []

    def copy(source, at, to, size):
        copies.append(
            pltpu.make_async_copy(
                source.at[pl.ds(at, size)], out.at[pl.ds(to, size)], done.at[len(copies)]
            )
        )
        copies[-1].start()

    for at in range(0, split, BLOCK):
        copy(held, at, at, min(BLOCK, split - at))

    def step(l, total):
        total = total + (anomaly[split + l + width - 1] - anomaly[split + l - 1])
        last[l] = (total * scale)[:days]
        return total

    total = lax.fori_loop(
        split - 1,
        split - 1 + width,
        lambda l, t: t + anomaly[l],
        jnp.zeros(anomaly.shape[1:], jnp.float32),
    )
    for at in range(0, count, BLOCK):
        size = min(BLOCK, count - at)
        total = lax.fori_loop(at, at + size, step, total)
        copy(last, at, split + at, size)
    for started in copies:
        started.wait()


def local(counts, field):
    days, lons, cols = field.shape
    x = jnp.transpose(field, (1, 0, 2))
    edges, middle = plan(lons)
    steps = len(edges) + len(middle)
    half = LON_HALF
    split = middle[-1][0] - half
    held, anomaly = pl.pallas_call(
        functools.partial(kernel, counts),
        out_shape=(
            pltpu.VMEM((split, days, cols), jnp.float32),
            pltpu.VMEM((lons + 2 * half, 3 * ROWS, cols), jnp.float32),
        ),
        in_specs=[pl.BlockSpec(memory_space=pltpu.HBM)],
        out_specs=(
            pl.BlockSpec(memory_space=pltpu.VMEM),
            pl.BlockSpec(memory_space=pltpu.VMEM),
        ),
        scratch_shapes=[
            pltpu.VMEM((lons, days, cols), jnp.bfloat16),
            pltpu.VMEM((lons, 2 * ROWS, cols), jnp.bfloat16),
            pltpu.VMEM((lons, 2 * ROWS, cols), jnp.bfloat16),
            pltpu.VMEM((lons, DAY_HALF, cols), jnp.bfloat16),
            pltpu.VMEM((lons, ROWS, cols), jnp.bfloat16),
            pltpu.VMEM((half, 3 * ROWS, cols), jnp.bfloat16),
            pltpu.VMEM((half, DAY_HALF, cols), jnp.bfloat16),
            pltpu.VMEM((half, 2 * ROWS, cols), jnp.bfloat16),
            pltpu.VMEM((half, 2 * ROWS, cols), jnp.bfloat16),
            pltpu.VMEM((half, ROWS, cols), jnp.bfloat16),
            pltpu.VMEM((SHARE, ROWS, cols), jnp.bfloat16),
            pltpu.SemaphoreType.DMA((lons // BLOCK,)),
            pltpu.SemaphoreType.DMA((2, steps)),
            pltpu.SemaphoreType.DMA((2, steps)),
            pltpu.SemaphoreType.DMA((lons // BLOCK,)),
            pltpu.SemaphoreType.DMA((lons // BLOCK,)),
            pltpu.SemaphoreType.DMA((4,)),
            pltpu.SemaphoreType.DMA((4,)),
            pltpu.SemaphoreType.DMA((11,)),
            pltpu.SemaphoreType.DMA((11,)),
            pltpu.SemaphoreType.REGULAR,
            pltpu.SemaphoreType.REGULAR,
            pltpu.SemaphoreType.REGULAR,
            pltpu.SemaphoreType.REGULAR,
            pltpu.SemaphoreType.REGULAR,
        ],
        compiler_params=pltpu.CompilerParams(
            collective_id=0, has_side_effects=True, vmem_limit_bytes=44 * 1024 * 1024
        ),
    )(x)
    count = lons - split
    z = pl.pallas_call(
        store,
        out_shape=pltpu.HBM((lons, days, cols), jnp.float32),
        in_specs=[pl.BlockSpec(memory_space=pltpu.VMEM)] * 2,
        out_specs=pl.BlockSpec(memory_space=pltpu.HBM),
        scratch_shapes=[
            pltpu.VMEM((count, days, cols), jnp.float32),
            pltpu.SemaphoreType.DMA((-(-split // BLOCK) - (-count // BLOCK),)),
        ],
        compiler_params=pltpu.CompilerParams(vmem_limit_bytes=8 * 1024 * 1024),
    )(
        pltpu.with_memory_space_constraint(held, pltpu.VMEM),
        pltpu.with_memory_space_constraint(anomaly, pltpu.VMEM),
    )
    return jnp.transpose(z, (1, 0, 2))


def solution(mesh):
    return jax.shard_map(
        functools.partial(local, (mesh.shape["day"], mesh.shape["lon"])),
        mesh=mesh,
        in_specs=(P("day", "lon", None),),
        out_specs=P("day", "lon", None),
        check_vma=False,
    )
```

```python
import functools

import jax
import jax.numpy as jnp
from jax import lax
from jax.experimental import pallas as pl
from jax.experimental.pallas import tpu as pltpu
from jax.sharding import PartitionSpec as P

DAY_HALF = 15
LON_HALF = 10
ROWS = 8
RUN = 8
BLOCK = 10
SHARE = 3
MESH = pl.DeviceIdType.MESH


def plan(lons):
    edges = [
        (0, ROWS, ROWS - 1),
        (lons - ROWS, ROWS, lons - ROWS),
        (ROWS, ROWS, 2 * ROWS - 1),
        (lons - 2 * ROWS, ROWS, lons - 2 * ROWS),
    ]
    middle = []
    for at in range(2 * ROWS, lons - 2 * ROWS, ROWS):
        size = min(ROWS, lons - 2 * ROWS - at)
        middle.append((at, size, at + ROWS - 1 if size == ROWS else None))
    return edges, middle


def hosts(group):
    at, size, rider = group
    if rider is None:
        return at, size
    return (at, size - 1) if rider > at else (at + 1, size - 1)


def grid(rows, cols):
    return (
        lax.broadcasted_iota(jnp.int32, (rows, cols), 0),
        lax.broadcasted_iota(jnp.int32, (rows, cols), 1),
    )


def ones(condition):
    return jnp.where(condition, 1.0, 0.0).astype(jnp.bfloat16)


def band(days, rows, shift):
    day, other = grid(days, rows)
    away = jnp.abs(day - other - shift)
    weight = jnp.where(away <= DAY_HALF, -1.0, 0.0)
    if shift == 0:
        weight = jnp.where(away == 0, 2.0 * DAY_HALF, weight)
    return weight.astype(jnp.bfloat16)


def dot(weight, values):
    return jnp.dot(weight, values, preferred_element_type=jnp.float32)


def kernel(
    counts, x, out, anomaly, far_days, own, after, before, packed,
    edge_own, edge_before, edge_after, edge_pass, edge_pack, relay,
    own_sem, far_send, far_recv, near_send, near_recv, lon_send, lon_recv,
    jump_send, jump_recv, near_ready, far_ready, lon_ready,
    chain_ready, jump_ready,
):
    lons, days, cols = x.shape
    half = LON_HALF
    day_count, lon_count = counts
    day, lon = lax.axis_index("day"), lax.axis_index("lon")
    day_next = lax.rem(day + 1, day_count)
    day_back = lax.rem(day + day_count - 1, day_count)
    lon_next = lax.rem(lon + 1, lon_count)
    lon_back = lax.rem(lon + lon_count - 1, lon_count)
    even = lax.rem(day, 2) == 0
    odd = jnp.logical_not(even)
    far = jnp.where(even, day_back, day_next)
    near = jnp.where(even, day_next, day_back)
    zone = lax.rem(lon, RUN)
    low = zone < RUN // 2
    reach = jnp.where(low, zone, RUN - 1 - zone)
    toward = jnp.where(low, lon_back, lon_next)
    low_jump = zone == 0
    high_jump = zone == RUN - 1
    jump = jnp.logical_or(low_jump, high_jump)
    peer = jnp.where(high_jump, lon_next, lon_back)
    edges, middle = plan(lons)
    order = edges + middle
    blocks = lons // BLOCK

    def load(b):
        rows = pl.ds(b * BLOCK, BLOCK)
        return pltpu.make_async_copy(x.at[rows], own.at[rows], own_sem.at[b])

    sequence = [0, blocks - 1, 1, blocks - 2, *range(2, blocks - 2)]
    for b in sequence:
        load(b).start()

    barrier = pltpu.get_barrier_semaphore()
    seat = lax.rem(day, 4)
    hub = seat == 0
    rest = jnp.logical_not(hub)

    def tell(semaphore, axis, *peers):
        for who in peers:
            pl.semaphore_signal(
                semaphore, inc=1, device_id={axis: who}, device_id_type=MESH
            )

    @pl.when(jnp.logical_or(hub, seat == 2))
    def _():
        tell(barrier, "day", day_back, day_next)

    @pl.when(seat == 1)
    def _():
        tell(barrier, "day", day_next)

    @pl.when(seat == 3)
    def _():
        tell(barrier, "day", day_back)

    @pl.when(rest)
    def _():
        pl.semaphore_wait(barrier, 2)

    @pl.when(seat == 1)
    def _():
        tell(near_ready, "day", day_back)

    @pl.when(seat == 3)
    def _():
        tell(far_ready, "day", day_next)

    @pl.when(hub)
    def _():
        pl.semaphore_wait(far_ready, 1)

    def remote(src, dst, send, recv, to):
        return pltpu.make_async_remote_copy(
            src_ref=src, dst_ref=dst, send_sem=send, recv_sem=recv,
            device_id=to, device_id_type=MESH,
        )

    start = pl.multiple_of(jnp.where(even, 0, ROWS), ROWS)

    def whole(n):
        at, size, _ = order[n]
        rows = pl.ds(at, size)
        return remote(
            (own if n else x).at[rows, pl.ds(start, ROWS)], far_days.at[rows, pl.ds(0, ROWS)],
            far_send.at[0, n], far_recv.at[0, n], {"day": far},
        )

    def second(n):
        rows = pl.ds(*hosts(order[n]))
        return remote(
            packed.at[rows], far_days.at[rows, pl.ds(ROWS, ROWS)],
            far_send.at[1, n], far_recv.at[1, n], {"day": far},
        )

    def near_even(b):
        rows = pl.ds(b * BLOCK, BLOCK)
        return remote(
            x.at[rows, pl.ds(ROWS, DAY_HALF)], before.at[rows],
            near_send.at[b], near_recv.at[b], {"day": near},
        )

    def near_odd(b):
        rows = pl.ds(b * BLOCK, BLOCK)
        return remote(
            x.at[rows, pl.ds(0, 2 * ROWS)], after.at[rows],
            near_send.at[b], near_recv.at[b], {"day": near},
        )

    edge = pl.ds(jnp.where(high_jump, lons - half, 0), half)
    across = {"lon": peer}
    corner = {"day": far, "lon": peer}

    row_of = pl.multiple_of(jnp.where(even, 2 * ROWS, 0), ROWS)
    relays = RUN // 2 - 1
    direct = half - relays * SHARE

    def jump_direct():
        rows = pl.ds(0, direct)
        return remote(edge_pack.at[rows], edge_own.at[rows, pl.ds(row_of, ROWS)],
                      jump_send.at[0], jump_recv.at[0], across)

    def jump_relay(r):
        by = lax.rem(jnp.where(high_jump, lon + 1 + r, lon + lon_count - 1 - r), lon_count)
        return remote(edge_pack.at[pl.ds(direct + (r - 1) * SHARE, SHARE)], relay,
                      jump_send.at[7 + r], jump_recv.at[1], {"lon": by})

    def relay_out(r):
        rows = pl.ds(direct + (r - 1) * SHARE, SHARE)
        return remote(relay, edge_own.at[rows, pl.ds(row_of, ROWS)],
                      jump_send.at[1], jump_recv.at[7 + r],
                      {"lon": jnp.where(low, lon - reach, lon + reach)})

    def corner_even():
        return [
            remote(x.at[edge, pl.ds(0, 2 * ROWS)], edge_after,
                   jump_send.at[2], jump_recv.at[2], corner),
            remote(far_days.at[edge], edge_own.at[:, pl.ds(ROWS, 2 * ROWS)],
                   jump_send.at[3], jump_recv.at[3], corner),
        ]

    def corner_odd():
        return [
            remote(x.at[edge, pl.ds(ROWS, DAY_HALF)], edge_before,
                   jump_send.at[4], jump_recv.at[4], corner),
            remote(far_days.at[edge], edge_own.at[:, pl.ds(0, 2 * ROWS)],
                   jump_send.at[5], jump_recv.at[5], corner),
        ]

    def pass_even():
        return remote(edge_own.at[:, pl.ds(ROWS, 2 * ROWS)], edge_pass,
                      jump_send.at[6], jump_recv.at[6], {"day": near})

    def pass_odd():
        return remote(edge_own.at[:, pl.ds(0, 2 * ROWS)], edge_after,
                      jump_send.at[7], jump_recv.at[7], {"day": near})

    jump_is_even = jnp.logical_and(jump, even)
    jump_is_odd = jnp.logical_and(jump, odd)

    waited = [0]

    def loaded(count):
        while waited[0] < count:
            load(sequence[waited[0]]).wait()
            waited[0] += 1

    for n in range(len(edges)):
        if n:
            loaded(n + 1)
        whole(n).start()

    @pl.when(hub)
    def _():
        pl.semaphore_wait(near_ready, 1)
        tell(barrier, "lon", lon_back, lon_next)

    @pl.when(even)
    def _():
        for b in range(blocks):
            near_even(b).start()

    @pl.when(odd)
    def _():
        for b in range(blocks):
            near_odd(b).start()

    place, col = grid(ROWS, days)
    part = DAY_HALF - ROWS
    first = jnp.where(even, ROWS, 2 * ROWS)
    keep = ones((place < part) & (col == first + place))

    def pack(n):
        at, size = hosts(order[n])
        rider = order[n][2]
        for i in range(size):
            tile = dot(keep, own[at + i])
            if rider is not None:
                ride = ones((place == part) & (col == first + i))
                tile = tile + dot(ride, own[rider])
            packed[at + i] = tile.astype(jnp.bfloat16)

    for n in range(len(order)):
        at, size, _ = order[n]
        if n >= len(edges):
            last = min((at + size - 1) // BLOCK, blocks - 3)
            loaded(max(4, sequence.index(last) + 1))
        if n >= len(edges):
            whole(n).start()
        pack(n)
        if n > 0:
            second(n - 1).start()
    loaded(blocks)
    own_band = band(3 * ROWS, days, 0)
    before_band = band(3 * ROWS, DAY_HALF, -DAY_HALF)
    after_band = band(3 * ROWS, 2 * ROWS, days)
    second(len(order) - 1).start()

    @pl.when(jump)
    def _():
        take = ones(col == jnp.where(even, DAY_HALF, 0) + place)
        for i in range(half):
            edge_pack[i] = dot(take, own[edge.start + i]).astype(jnp.bfloat16)

    @pl.when(even)
    def _():
        @pl.loop(0, blocks)
        def _(b):
            near_odd(b).wait_recv()
            for i in range(BLOCK):
                l = b * BLOCK + i
                anomaly[l + half] = dot(own_band, own[l]) + dot(after_band, after[l])

    @pl.when(odd)
    def _():
        @pl.loop(0, blocks)
        def _(b):
            near_even(b).wait_recv()
            for i in range(BLOCK):
                l = b * BLOCK + i
                anomaly[l + half] = dot(own_band, own[l]) + dot(before_band, before[l])

    @pl.when(hub)
    def _():
        pl.semaphore_wait(barrier, 2)
        tell(lon_ready, "day", day_back, day_next)

    @pl.when(seat == 1)
    def _():
        pl.semaphore_wait(lon_ready, 1)
        tell(lon_ready, "day", day_next)

    @pl.when(seat == 3)
    def _():
        pl.semaphore_wait(lon_ready, 1)
        tell(lon_ready, "day", day_back)

    @pl.when(seat == 2)
    def _():
        pl.semaphore_wait(lon_ready, 2)

    @pl.when(jump_is_even)
    def _():
        corner_even()[0].start()

    @pl.when(jump_is_odd)
    def _():
        corner_odd()[0].start()

    @pl.when(reach == 2)
    def _():
        tell(chain_ready, "lon", toward)

    @pl.when(reach == 1)
    def _():
        pl.semaphore_wait(chain_ready, 1)
        tell(chain_ready, "lon", toward)

    @pl.when(jump)
    def _():
        pl.semaphore_wait(chain_ready, 1)
        tell(jump_ready, "lon", toward)
        pl.semaphore_wait(jump_ready, 1)
        jump_direct().start()
        for r in range(1, relays + 1):
            jump_relay(r).start()

    row, other = grid(2 * ROWS, 2 * ROWS)
    way = jnp.where(even, 1, -1)
    far_band = jnp.where(
        ((other - row) * way >= 0) & (other < DAY_HALF), -1.0, 0.0
    ).astype(jnp.bfloat16)
    touched = pl.ds(start, 2 * ROWS)
    lane, source = grid(ROWS, ROWS)

    def daily(n):
        at, size, rider = order[n]
        whole(n).wait_recv()
        second(n).wait_recv()
        if rider is not None:
            host, count = hosts(order[n])
            tile = jnp.zeros((ROWS, cols), jnp.float32)
            for i in range(count):
                take = ones((lane == i) & (source == part))
                tile = tile + dot(take, far_days[host + i, pl.ds(ROWS, ROWS)])
            far_days[rider, pl.ds(ROWS, ROWS)] = tile.astype(jnp.bfloat16)
        for l in range(at, at + size):
            anomaly[l + half, touched] += dot(far_band, far_days[l])

    pieces = [
        (0, ROWS), (lons - ROWS, ROWS), (ROWS, half - ROWS), (lons - half, half - ROWS),
    ]

    def shift(n):
        at, size = pieces[n]
        down = n % 2 == 0
        place = at + half + (lons if down else -lons)
        return remote(
            anomaly.at[pl.ds(at + half, size)], anomaly.at[pl.ds(place, size)],
            lon_send.at[n], lon_recv.at[n], {"lon": lon_back if down else lon_next},
        )

    def advance(n):
        daily(n)
        if 0 < n <= len(edges):
            stays = low_jump if (n - 1) % 2 == 0 else high_jump

            @pl.when(jnp.logical_not(stays))
            def _():
                shift(n - 1).start()

    for n in range(len(edges)):
        if n == 2:
            @pl.when(reach > 0)
            def _():
                jump_relay(1).wait_recv()
                relay_out(reach).start()
        advance(n)

    @pl.when(jump_is_even)
    def _():
        corner_even()[1].start()

    @pl.when(jump_is_odd)
    def _():
        corner_odd()[1].start()

    def pass_on():
        @pl.when(jump)
        def _():
            jump_direct().wait_recv()
            for r in range(1, relays + 1):
                relay_out(r).wait_recv()

        @pl.when(jump_is_even)
        def _():
            corner_odd()[1].wait_recv()
            pass_even().start()

        @pl.when(jump_is_odd)
        def _():
            corner_even()[1].wait_recv()
            pass_odd().start()

    def zonal_edges():
        day_of, slot = grid(3 * ROWS, 3 * ROWS)
        held = jnp.where(even & (slot > DAY_HALF), slot - 1, slot)
        spare = jnp.where(even, DAY_HALF, days)
        away = jnp.abs(day_of - held)
        edge_band = jnp.where(away <= DAY_HALF, -1.0, 0.0)
        edge_band = jnp.where(away == 0, 2.0 * DAY_HALF, edge_band)
        edge_band = jnp.where(slot == spare, 0.0, edge_band).astype(jnp.bfloat16)
        to = jnp.where(high_jump, lons + half, 0)

        @pl.when(jump_is_even)
        def _():
            corner_odd()[0].wait_recv()
            pass_odd().wait_recv()
            for i in range(half):
                anomaly[to + i] = (
                    dot(edge_band, edge_own[i])
                    + dot(before_band, edge_before[i])
                    + dot(after_band, edge_after[i])
                )

        @pl.when(jump_is_odd)
        def _():
            corner_even()[0].wait_recv()
            pass_even().wait_recv()
            day_of, slot = grid(3 * ROWS, 2 * ROWS)
            held = jnp.where(slot > part, slot - 1, slot)
            pass_band = jnp.where(
                (held >= day_of) & (slot != part), -1.0, 0.0
            ).astype(jnp.bfloat16)
            for i in range(half):
                anomaly[to + i] = (
                    dot(edge_band, edge_own[i])
                    + dot(pass_band, edge_pass[i])
                    + dot(after_band, edge_after[i])
                )

        @pl.when(jnp.logical_not(high_jump))
        def _():
            shift(0).wait_recv()
            shift(2).wait_recv()

        @pl.when(jnp.logical_not(low_jump))
        def _():
            shift(1).wait_recv()
            shift(3).wait_recv()

    scale = 1.0 / ((2 * DAY_HALF + 1) * (2 * half + 1))
    width = 2 * half + 1

    def up_to(lo, hi, total):
        def step(l, total):
            total = total + (anomaly[l + width - 1] - anomaly[l - 1])
            out[l] = (total * scale)[:days]
            return total

        return lax.fori_loop(lo, hi, step, total)

    def back(step, total):
        l = half - 1 - step
        total = total + (anomaly[l] - anomaly[l + width])
        out[l] = (total * scale)[:days]
        return total

    def finish_edges(total):
        zonal_edges()
        lax.fori_loop(0, half, back, total)

    early = jnp.logical_or(seat == 0, seat == 3)
    late = jnp.logical_not(early)
    steps = len(order)
    total = None
    done = half
    for n in range(len(edges), steps):
        end = n == steps - 1
        if n == steps - 4:
            pl.when(late)(pass_on)
        if n == steps - 2:
            pl.when(late)(functools.partial(finish_edges, first_total))
        if end:
            whole(n).wait_recv()
            second(n).wait_recv()
            continue
        advance(n)
        ready = order[n][0] + order[n][1] - half
        if ready <= half:
            continue
        if total is None:
            total = lax.fori_loop(
                half,
                half + width,
                lambda l, t: t + anomaly[l],
                jnp.zeros((3 * ROWS, cols), jnp.float32),
            )
            out[half] = (total * scale)[:days]
            first_total = total
            done = half + 1
        total = up_to(done, ready, total)
        done = ready

    @pl.when(early)
    def _():
        pass_on()
        finish_edges(first_total)

    for n in range(steps):
        whole(n).wait_send()
        second(n).wait_send()

    @pl.when(even)
    def _():
        for b in range(blocks):
            near_even(b).wait_send()

    @pl.when(odd)
    def _():
        for b in range(blocks):
            near_odd(b).wait_send()

    for n in range(len(pieces)):
        stays = low_jump if n % 2 == 0 else high_jump

        @pl.when(jnp.logical_not(stays))
        def _():
            shift(n).wait_send()

    @pl.when(jump)
    def _():
        jump_direct().wait_send()
        for r in range(1, relays + 1):
            jump_relay(r).wait_send()

    @pl.when(reach > 0)
    def _():
        relay_out(reach).wait_send()

    @pl.when(jump_is_even)
    def _():
        for copy in (*corner_even(), pass_even()):
            copy.wait_send()

    @pl.when(jump_is_odd)
    def _():
        for copy in (*corner_odd(), pass_odd()):
            copy.wait_send()


def store(final, late, held, anomaly, far_days, out, last, part, done):
    split, days, _ = held.shape
    count = last.shape[0]
    half = LON_HALF
    width = 2 * half + 1
    scale = 1.0 / ((2 * DAY_HALF + 1) * width)
    copies = []

    def copy(source, at, to, size):
        copies.append(
            pltpu.make_async_copy(
                source.at[pl.ds(at, size)], out.at[pl.ds(to, size)], done.at[len(copies)]
            )
        )
        copies[-1].start()

    for at in range(0, split, BLOCK):
        copy(held, at, at, min(BLOCK, split - at))

    day, other = grid(3 * ROWS, 2 * ROWS)
    even = lax.rem(lax.axis_index("day"), 2) == 0
    first = jnp.where(even, day - other, other - day + ROWS)
    far_band = jnp.where((first <= 0) & (other < DAY_HALF), -1.0, 0.0)
    far_band = far_band.astype(jnp.bfloat16)
    for i in range(late):
        part[i] = dot(far_band, far_days[final + i])

    def step(l, total):
        total = total + (anomaly[split + l + width - 1] - anomaly[split + l - 1])
        last[l] = (total * scale)[:days]
        return total

    total = lax.fori_loop(
        split - 1,
        split - 1 + width,
        lambda l, t: t + anomaly[l],
        jnp.zeros(anomaly.shape[1:], jnp.float32),
    )
    done_to, sent = 0, 0
    for at, sign in sorted(
        [(i, 1) for i in range(late)]
        + [(width + i, -1) for i in range(late)]
        + [(count, 0)]
    ):
        total = lax.fori_loop(done_to, at, step, total)
        if sign:
            fresh = part[at] if sign > 0 else -part[at - width]
            total = step(at, total + fresh)
            done_to = at + 1
        if sent + BLOCK <= at or at == count:
            copy(last, sent, split + sent, at - sent)
            sent = at
    for started in copies:
        started.wait()


def local(counts, field):
    days, lons, cols = field.shape
    x = jnp.transpose(field, (1, 0, 2))
    edges, middle = plan(lons)
    steps = len(edges) + len(middle)
    half = LON_HALF
    split = middle[-1][0] - half
    held, anomaly, far_days = pl.pallas_call(
        functools.partial(kernel, counts),
        out_shape=(
            pltpu.VMEM((split, days, cols), jnp.float32),
            pltpu.VMEM((lons + 2 * half, 3 * ROWS, cols), jnp.float32),
            pltpu.VMEM((lons, 2 * ROWS, cols), jnp.bfloat16),
        ),
        in_specs=[pl.BlockSpec(memory_space=pltpu.HBM)],
        out_specs=(pl.BlockSpec(memory_space=pltpu.VMEM),) * 3,
        scratch_shapes=[
            pltpu.VMEM((lons, days, cols), jnp.bfloat16),
            pltpu.VMEM((lons, 2 * ROWS, cols), jnp.bfloat16),
            pltpu.VMEM((lons, DAY_HALF, cols), jnp.bfloat16),
            pltpu.VMEM((lons, ROWS, cols), jnp.bfloat16),
            pltpu.VMEM((half, 3 * ROWS, cols), jnp.bfloat16),
            pltpu.VMEM((half, DAY_HALF, cols), jnp.bfloat16),
            pltpu.VMEM((half, 2 * ROWS, cols), jnp.bfloat16),
            pltpu.VMEM((half, 2 * ROWS, cols), jnp.bfloat16),
            pltpu.VMEM((half, ROWS, cols), jnp.bfloat16),
            pltpu.VMEM((SHARE, ROWS, cols), jnp.bfloat16),
            pltpu.SemaphoreType.DMA((lons // BLOCK,)),
            pltpu.SemaphoreType.DMA((2, steps)),
            pltpu.SemaphoreType.DMA((2, steps)),
            pltpu.SemaphoreType.DMA((lons // BLOCK,)),
            pltpu.SemaphoreType.DMA((lons // BLOCK,)),
            pltpu.SemaphoreType.DMA((4,)),
            pltpu.SemaphoreType.DMA((4,)),
            pltpu.SemaphoreType.DMA((11,)),
            pltpu.SemaphoreType.DMA((11,)),
            pltpu.SemaphoreType.REGULAR,
            pltpu.SemaphoreType.REGULAR,
            pltpu.SemaphoreType.REGULAR,
            pltpu.SemaphoreType.REGULAR,
            pltpu.SemaphoreType.REGULAR,
        ],
        compiler_params=pltpu.CompilerParams(
            collective_id=0, has_side_effects=True, vmem_limit_bytes=40 * 1024 * 1024
        ),
    )(x)
    count = lons - split
    z = pl.pallas_call(
        functools.partial(store, *middle[-1][:2]),
        out_shape=pltpu.HBM((lons, days, cols), jnp.float32),
        in_specs=[pl.BlockSpec(memory_space=pltpu.VMEM)] * 3,
        out_specs=pl.BlockSpec(memory_space=pltpu.HBM),
        scratch_shapes=[
            pltpu.VMEM((count, days, cols), jnp.float32),
            pltpu.VMEM((middle[-1][1], 3 * ROWS, cols), jnp.float32),
            pltpu.SemaphoreType.DMA((-(-split // BLOCK) - (-count // BLOCK),)),
        ],
        compiler_params=pltpu.CompilerParams(vmem_limit_bytes=8 * 1024 * 1024),
    )(
        pltpu.with_memory_space_constraint(held, pltpu.VMEM),
        pltpu.with_memory_space_constraint(anomaly, pltpu.VMEM),
        pltpu.with_memory_space_constraint(far_days, pltpu.VMEM),
    )
    return jnp.transpose(z, (1, 0, 2))


def solution(mesh):
    return jax.shard_map(
        functools.partial(local, (mesh.shape["day"], mesh.shape["lon"])),
        mesh=mesh,
        in_specs=(P("day", "lon", None),),
        out_specs=P("day", "lon", None),
        check_vma=False,
    )
```

```python
import functools

import jax
import jax.numpy as jnp
from jax import lax
from jax.experimental import pallas as pl
from jax.experimental.pallas import tpu as pltpu
from jax.sharding import PartitionSpec as P

DAY_HALF = 15
LON_HALF = 10
ROWS = 8
RUN = 8
BLOCK = 10
SHARE = 3
MESH = pl.DeviceIdType.MESH


def plan(lons):
    edges = [
        (0, ROWS, ROWS - 1),
        (lons - ROWS, ROWS, lons - ROWS),
        (ROWS, ROWS, 2 * ROWS - 1),
        (lons - 2 * ROWS, ROWS, lons - 2 * ROWS),
    ]
    middle = []
    for at in range(2 * ROWS, lons - 2 * ROWS, ROWS):
        size = min(ROWS, lons - 2 * ROWS - at)
        middle.append((at, size, at + ROWS - 1 if size == ROWS else None))
    return edges, middle


def hosts(group):
    at, size, rider = group
    if rider is None:
        return at, size
    return (at, size - 1) if rider > at else (at + 1, size - 1)


def grid(rows, cols):
    return (
        lax.broadcasted_iota(jnp.int32, (rows, cols), 0),
        lax.broadcasted_iota(jnp.int32, (rows, cols), 1),
    )


def ones(condition):
    return jnp.where(condition, 1.0, 0.0).astype(jnp.bfloat16)


def band(days, rows, shift):
    day, other = grid(days, rows)
    away = jnp.abs(day - other - shift)
    weight = jnp.where(away <= DAY_HALF, -1.0, 0.0)
    if shift == 0:
        weight = jnp.where(away == 0, 2.0 * DAY_HALF, weight)
    return weight.astype(jnp.bfloat16)


def dot(weight, values):
    return jnp.dot(weight, values, preferred_element_type=jnp.float32)


def kernel(
    counts, x, out, anomaly, far_days, own, after, before, packed,
    edge_own, edge_before, edge_after, edge_pass, edge_pack, relay,
    own_sem, far_send, far_recv, near_send, near_recv, lon_send, lon_recv,
    jump_send, jump_recv, near_ready, far_ready, lon_ready,
    chain_ready, jump_ready,
):
    lons, days, cols = x.shape
    half = LON_HALF
    day_count, lon_count = counts
    day, lon = lax.axis_index("day"), lax.axis_index("lon")
    day_next = lax.rem(day + 1, day_count)
    day_back = lax.rem(day + day_count - 1, day_count)
    lon_next = lax.rem(lon + 1, lon_count)
    lon_back = lax.rem(lon + lon_count - 1, lon_count)
    even = lax.rem(day, 2) == 0
    odd = jnp.logical_not(even)
    far = jnp.where(even, day_back, day_next)
    near = jnp.where(even, day_next, day_back)
    zone = lax.rem(lon, RUN)
    low = zone < RUN // 2
    reach = jnp.where(low, zone, RUN - 1 - zone)
    toward = jnp.where(low, lon_back, lon_next)
    low_jump = zone == 0
    high_jump = zone == RUN - 1
    jump = jnp.logical_or(low_jump, high_jump)
    peer = jnp.where(high_jump, lon_next, lon_back)
    edges, middle = plan(lons)
    order = edges + middle
    blocks = lons // BLOCK

    def load(b):
        rows = pl.ds(b * BLOCK, BLOCK)
        return pltpu.make_async_copy(x.at[rows], own.at[rows], own_sem.at[b])

    sequence = [0, blocks - 1, 1, blocks - 2, *range(2, blocks - 2)]
    for b in sequence:
        load(b).start()

    barrier = pltpu.get_barrier_semaphore()
    seat = lax.rem(day, 4)
    hub = seat == 0
    rest = jnp.logical_not(hub)

    def tell(semaphore, axis, *peers):
        for who in peers:
            pl.semaphore_signal(
                semaphore, inc=1, device_id={axis: who}, device_id_type=MESH
            )

    @pl.when(jnp.logical_or(hub, seat == 2))
    def _():
        tell(barrier, "day", day_back, day_next)

    @pl.when(seat == 1)
    def _():
        tell(barrier, "day", day_next)

    @pl.when(seat == 3)
    def _():
        tell(barrier, "day", day_back)

    @pl.when(rest)
    def _():
        pl.semaphore_wait(barrier, 2)

    @pl.when(seat == 1)
    def _():
        tell(near_ready, "day", day_back)

    @pl.when(seat == 3)
    def _():
        tell(far_ready, "day", day_next)

    @pl.when(hub)
    def _():
        pl.semaphore_wait(far_ready, 1)

    def remote(src, dst, send, recv, to):
        return pltpu.make_async_remote_copy(
            src_ref=src, dst_ref=dst, send_sem=send, recv_sem=recv,
            device_id=to, device_id_type=MESH,
        )

    start = pl.multiple_of(jnp.where(even, 0, ROWS), ROWS)

    def whole(n, days_of=own):
        at, size, _ = order[n]
        rows = pl.ds(at, size)
        return remote(
            days_of.at[rows, pl.ds(start, ROWS)], far_days.at[rows, pl.ds(0, ROWS)],
            far_send.at[0, n], far_recv.at[0, n], {"day": far},
        )

    def second(n):
        rows = pl.ds(*hosts(order[n]))
        return remote(
            packed.at[rows], far_days.at[rows, pl.ds(ROWS, ROWS)],
            far_send.at[1, n], far_recv.at[1, n], {"day": far},
        )

    def near_even(b):
        rows = pl.ds(b * BLOCK, BLOCK)
        return remote(
            x.at[rows, pl.ds(ROWS, DAY_HALF)], before.at[rows],
            near_send.at[b], near_recv.at[b], {"day": near},
        )

    def near_odd(b):
        rows = pl.ds(b * BLOCK, BLOCK)
        return remote(
            x.at[rows, pl.ds(0, 2 * ROWS)], after.at[rows],
            near_send.at[b], near_recv.at[b], {"day": near},
        )

    edge = pl.ds(jnp.where(high_jump, lons - half, 0), half)
    across = {"lon": peer}
    corner = {"day": far, "lon": peer}

    row_of = pl.multiple_of(jnp.where(even, 2 * ROWS, 0), ROWS)
    relays = RUN // 2 - 1
    direct = half - relays * SHARE

    def jump_direct():
        rows = pl.ds(0, direct)
        return remote(edge_pack.at[rows], edge_own.at[rows, pl.ds(row_of, ROWS)],
                      jump_send.at[0], jump_recv.at[0], across)

    def jump_relay(r):
        by = lax.rem(jnp.where(high_jump, lon + 1 + r, lon + lon_count - 1 - r), lon_count)
        return remote(edge_pack.at[pl.ds(direct + (r - 1) * SHARE, SHARE)], relay,
                      jump_send.at[7 + r], jump_recv.at[1], {"lon": by})

    def relay_out(r):
        rows = pl.ds(direct + (r - 1) * SHARE, SHARE)
        return remote(relay, edge_own.at[rows, pl.ds(row_of, ROWS)],
                      jump_send.at[1], jump_recv.at[7 + r],
                      {"lon": jnp.where(low, lon - reach, lon + reach)})

    def corner_even():
        return [
            remote(x.at[edge, pl.ds(0, 2 * ROWS)], edge_after,
                   jump_send.at[2], jump_recv.at[2], corner),
            remote(far_days.at[edge], edge_own.at[:, pl.ds(ROWS, 2 * ROWS)],
                   jump_send.at[3], jump_recv.at[3], corner),
        ]

    def corner_odd():
        return [
            remote(x.at[edge, pl.ds(ROWS, DAY_HALF)], edge_before,
                   jump_send.at[4], jump_recv.at[4], corner),
            remote(far_days.at[edge], edge_own.at[:, pl.ds(0, 2 * ROWS)],
                   jump_send.at[5], jump_recv.at[5], corner),
        ]

    def pass_even():
        return remote(edge_own.at[:, pl.ds(ROWS, 2 * ROWS)], edge_pass,
                      jump_send.at[6], jump_recv.at[6], {"day": near})

    def pass_odd():
        return remote(edge_own.at[:, pl.ds(0, 2 * ROWS)], edge_after,
                      jump_send.at[7], jump_recv.at[7], {"day": near})

    jump_is_even = jnp.logical_and(jump, even)
    jump_is_odd = jnp.logical_and(jump, odd)

    @pl.when(seat == 2)
    def _():
        for n in range(len(edges)):
            whole(n, x).start()

    waited = [0]

    def loaded(count):
        while waited[0] < count:
            load(sequence[waited[0]]).wait()
            waited[0] += 1

    for n in range(len(edges)):
        loaded(n + 1)

        @pl.when(seat != 2)
        def _():
            whole(n).start()

    @pl.when(hub)
    def _():
        pl.semaphore_wait(near_ready, 1)
        tell(barrier, "lon", lon_back, lon_next)

    @pl.when(even)
    def _():
        for b in range(blocks):
            near_even(b).start()

    @pl.when(odd)
    def _():
        for b in range(blocks):
            near_odd(b).start()

    place, col = grid(ROWS, days)
    part = DAY_HALF - ROWS
    first = jnp.where(even, ROWS, 2 * ROWS)
    keep = ones((place < part) & (col == first + place))

    def pack(n):
        at, size = hosts(order[n])
        rider = order[n][2]
        for i in range(size):
            tile = dot(keep, own[at + i])
            if rider is not None:
                ride = ones((place == part) & (col == first + i))
                tile = tile + dot(ride, own[rider])
            packed[at + i] = tile.astype(jnp.bfloat16)

    for n in range(len(order)):
        at, size, _ = order[n]
        if n >= len(edges):
            last = min((at + size - 1) // BLOCK, blocks - 3)
            loaded(max(4, sequence.index(last) + 1))
        if n >= len(edges):
            whole(n).start()
        pack(n)
        if n > 0:
            second(n - 1).start()
    loaded(blocks)
    own_band = band(3 * ROWS, days, 0)
    before_band = band(3 * ROWS, DAY_HALF, -DAY_HALF)
    after_band = band(3 * ROWS, 2 * ROWS, days)
    second(len(order) - 1).start()

    @pl.when(jump)
    def _():
        take = ones(col == jnp.where(even, DAY_HALF, 0) + place)
        for i in range(half):
            edge_pack[i] = dot(take, own[edge.start + i]).astype(jnp.bfloat16)

    @pl.when(even)
    def _():
        @pl.loop(0, blocks)
        def _(b):
            near_odd(b).wait_recv()
            for i in range(BLOCK):
                l = b * BLOCK + i
                anomaly[l + half] = dot(own_band, own[l]) + dot(after_band, after[l])

    @pl.when(odd)
    def _():
        @pl.loop(0, blocks)
        def _(b):
            near_even(b).wait_recv()
            for i in range(BLOCK):
                l = b * BLOCK + i
                anomaly[l + half] = dot(own_band, own[l]) + dot(before_band, before[l])

    @pl.when(hub)
    def _():
        pl.semaphore_wait(barrier, 2)
        tell(lon_ready, "day", day_back, day_next)

    @pl.when(seat == 1)
    def _():
        pl.semaphore_wait(lon_ready, 1)
        tell(lon_ready, "day", day_next)

    @pl.when(seat == 3)
    def _():
        pl.semaphore_wait(lon_ready, 1)
        tell(lon_ready, "day", day_back)

    @pl.when(seat == 2)
    def _():
        pl.semaphore_wait(lon_ready, 2)

    @pl.when(jump_is_even)
    def _():
        corner_even()[0].start()

    @pl.when(jump_is_odd)
    def _():
        corner_odd()[0].start()

    @pl.when(reach == 2)
    def _():
        tell(chain_ready, "lon", toward)

    @pl.when(reach == 1)
    def _():
        pl.semaphore_wait(chain_ready, 1)
        tell(chain_ready, "lon", toward)

    @pl.when(jump)
    def _():
        pl.semaphore_wait(chain_ready, 1)
        tell(jump_ready, "lon", toward)
        pl.semaphore_wait(jump_ready, 1)
        jump_direct().start()
        for r in range(1, relays + 1):
            jump_relay(r).start()

    row, other = grid(2 * ROWS, 2 * ROWS)
    way = jnp.where(even, 1, -1)
    far_band = jnp.where(
        ((other - row) * way >= 0) & (other < DAY_HALF), -1.0, 0.0
    ).astype(jnp.bfloat16)
    touched = pl.ds(start, 2 * ROWS)
    lane, source = grid(ROWS, ROWS)

    def daily(n):
        at, size, rider = order[n]
        whole(n).wait_recv()
        second(n).wait_recv()
        if rider is not None:
            host, count = hosts(order[n])
            tile = jnp.zeros((ROWS, cols), jnp.float32)
            for i in range(count):
                take = ones((lane == i) & (source == part))
                tile = tile + dot(take, far_days[host + i, pl.ds(ROWS, ROWS)])
            far_days[rider, pl.ds(ROWS, ROWS)] = tile.astype(jnp.bfloat16)
        for l in range(at, at + size):
            anomaly[l + half, touched] += dot(far_band, far_days[l])

    pieces = [
        (0, ROWS), (lons - ROWS, ROWS), (ROWS, half - ROWS), (lons - half, half - ROWS),
    ]

    def shift(n):
        at, size = pieces[n]
        down = n % 2 == 0
        place = at + half + (lons if down else -lons)
        return remote(
            anomaly.at[pl.ds(at + half, size)], anomaly.at[pl.ds(place, size)],
            lon_send.at[n], lon_recv.at[n], {"lon": lon_back if down else lon_next},
        )

    def advance(n):
        daily(n)
        if 0 < n <= len(edges):
            stays = low_jump if (n - 1) % 2 == 0 else high_jump

            @pl.when(jnp.logical_not(stays))
            def _():
                shift(n - 1).start()

    for n in range(len(edges)):
        if n == 2:
            @pl.when(reach > 0)
            def _():
                jump_relay(1).wait_recv()
                relay_out(reach).start()
        advance(n)

    @pl.when(jump_is_even)
    def _():
        corner_even()[1].start()

    @pl.when(jump_is_odd)
    def _():
        corner_odd()[1].start()

    def pass_on():
        @pl.when(jump)
        def _():
            jump_direct().wait_recv()
            for r in range(1, relays + 1):
                relay_out(r).wait_recv()

        @pl.when(jump_is_even)
        def _():
            corner_odd()[1].wait_recv()
            pass_even().start()

        @pl.when(jump_is_odd)
        def _():
            corner_even()[1].wait_recv()
            pass_odd().start()

    def zonal_edges():
        day_of, slot = grid(3 * ROWS, 3 * ROWS)
        held = jnp.where(even & (slot > DAY_HALF), slot - 1, slot)
        spare = jnp.where(even, DAY_HALF, days)
        away = jnp.abs(day_of - held)
        edge_band = jnp.where(away <= DAY_HALF, -1.0, 0.0)
        edge_band = jnp.where(away == 0, 2.0 * DAY_HALF, edge_band)
        edge_band = jnp.where(slot == spare, 0.0, edge_band).astype(jnp.bfloat16)
        to = jnp.where(high_jump, lons + half, 0)

        @pl.when(jump_is_even)
        def _():
            corner_odd()[0].wait_recv()
            pass_odd().wait_recv()
            for i in range(half):
                anomaly[to + i] = (
                    dot(edge_band, edge_own[i])
                    + dot(before_band, edge_before[i])
                    + dot(after_band, edge_after[i])
                )

        @pl.when(jump_is_odd)
        def _():
            corner_even()[0].wait_recv()
            pass_even().wait_recv()
            day_of, slot = grid(3 * ROWS, 2 * ROWS)
            held = jnp.where(slot > part, slot - 1, slot)
            pass_band = jnp.where(
                (held >= day_of) & (slot != part), -1.0, 0.0
            ).astype(jnp.bfloat16)
            for i in range(half):
                anomaly[to + i] = (
                    dot(edge_band, edge_own[i])
                    + dot(pass_band, edge_pass[i])
                    + dot(after_band, edge_after[i])
                )

        @pl.when(jnp.logical_not(high_jump))
        def _():
            shift(0).wait_recv()
            shift(2).wait_recv()

        @pl.when(jnp.logical_not(low_jump))
        def _():
            shift(1).wait_recv()
            shift(3).wait_recv()

    scale = 1.0 / ((2 * DAY_HALF + 1) * (2 * half + 1))
    width = 2 * half + 1

    def up_to(lo, hi, total):
        def step(l, total):
            total = total + (anomaly[l + width - 1] - anomaly[l - 1])
            out[l] = (total * scale)[:days]
            return total

        return lax.fori_loop(lo, hi, step, total)

    def back(step, total):
        l = half - 1 - step
        total = total + (anomaly[l] - anomaly[l + width])
        out[l] = (total * scale)[:days]
        return total

    def finish_edges(total):
        zonal_edges()
        lax.fori_loop(0, half, back, total)

    early = jnp.logical_or(seat == 0, seat == 3)
    late = jnp.logical_not(early)
    steps = len(order)
    total = None
    done = half
    for n in range(len(edges), steps):
        end = n == steps - 1
        if n == steps - 4:
            pl.when(late)(pass_on)
        if n == steps - 2:
            pl.when(late)(functools.partial(finish_edges, first_total))
        if end:
            whole(n).wait_recv()
            second(n).wait_recv()
            continue
        advance(n)
        ready = order[n][0] + order[n][1] - half
        if ready <= half:
            continue
        if total is None:
            total = lax.fori_loop(
                half,
                half + width,
                lambda l, t: t + anomaly[l],
                jnp.zeros((3 * ROWS, cols), jnp.float32),
            )
            out[half] = (total * scale)[:days]
            first_total = total
            done = half + 1
        total = up_to(done, ready, total)
        done = ready

    @pl.when(early)
    def _():
        pass_on()
        finish_edges(first_total)

    for n in range(steps):
        whole(n).wait_send()
        second(n).wait_send()

    @pl.when(even)
    def _():
        for b in range(blocks):
            near_even(b).wait_send()

    @pl.when(odd)
    def _():
        for b in range(blocks):
            near_odd(b).wait_send()

    for n in range(len(pieces)):
        stays = low_jump if n % 2 == 0 else high_jump

        @pl.when(jnp.logical_not(stays))
        def _():
            shift(n).wait_send()

    @pl.when(jump)
    def _():
        jump_direct().wait_send()
        for r in range(1, relays + 1):
            jump_relay(r).wait_send()

    @pl.when(reach > 0)
    def _():
        relay_out(reach).wait_send()

    @pl.when(jump_is_even)
    def _():
        for copy in (*corner_even(), pass_even()):
            copy.wait_send()

    @pl.when(jump_is_odd)
    def _():
        for copy in (*corner_odd(), pass_odd()):
            copy.wait_send()


def store(final, late, held, anomaly, far_days, out, last, part, done):
    split, days, _ = held.shape
    count = last.shape[0]
    half = LON_HALF
    width = 2 * half + 1
    scale = 1.0 / ((2 * DAY_HALF + 1) * width)
    copies = []

    def copy(source, at, to, size):
        copies.append(
            pltpu.make_async_copy(
                source.at[pl.ds(at, size)], out.at[pl.ds(to, size)], done.at[len(copies)]
            )
        )
        copies[-1].start()

    for at in range(0, split, BLOCK):
        copy(held, at, at, min(BLOCK, split - at))

    day, other = grid(3 * ROWS, 2 * ROWS)
    even = lax.rem(lax.axis_index("day"), 2) == 0
    first = jnp.where(even, day - other, other - day + ROWS)
    far_band = jnp.where((first <= 0) & (other < DAY_HALF), -1.0, 0.0)
    far_band = far_band.astype(jnp.bfloat16)
    for i in range(late):
        part[i] = dot(far_band, far_days[final + i])

    def step(l, total):
        total = total + (anomaly[split + l + width - 1] - anomaly[split + l - 1])
        last[l] = (total * scale)[:days]
        return total

    total = lax.fori_loop(
        split - 1,
        split - 1 + width,
        lambda l, t: t + anomaly[l],
        jnp.zeros(anomaly.shape[1:], jnp.float32),
    )
    done_to, sent = 0, 0
    for at, sign in sorted(
        [(i, 1) for i in range(late)]
        + [(width + i, -1) for i in range(late)]
        + [(count, 0)]
    ):
        total = lax.fori_loop(done_to, at, step, total)
        if sign:
            fresh = part[at] if sign > 0 else -part[at - width]
            total = step(at, total + fresh)
            done_to = at + 1
        if sent + BLOCK <= at or at == count:
            copy(last, sent, split + sent, at - sent)
            sent = at
    for started in copies:
        started.wait()


def local(counts, field):
    days, lons, cols = field.shape
    x = jnp.transpose(field, (1, 0, 2))
    edges, middle = plan(lons)
    steps = len(edges) + len(middle)
    half = LON_HALF
    split = middle[-1][0] - half
    held, anomaly, far_days = pl.pallas_call(
        functools.partial(kernel, counts),
        out_shape=(
            pltpu.VMEM((split, days, cols), jnp.float32),
            pltpu.VMEM((lons + 2 * half, 3 * ROWS, cols), jnp.float32),
            pltpu.VMEM((lons, 2 * ROWS, cols), jnp.bfloat16),
        ),
        in_specs=[pl.BlockSpec(memory_space=pltpu.HBM)],
        out_specs=(pl.BlockSpec(memory_space=pltpu.VMEM),) * 3,
        scratch_shapes=[
            pltpu.VMEM((lons, days, cols), jnp.bfloat16),
            pltpu.VMEM((lons, 2 * ROWS, cols), jnp.bfloat16),
            pltpu.VMEM((lons, DAY_HALF, cols), jnp.bfloat16),
            pltpu.VMEM((lons, ROWS, cols), jnp.bfloat16),
            pltpu.VMEM((half, 3 * ROWS, cols), jnp.bfloat16),
            pltpu.VMEM((half, DAY_HALF, cols), jnp.bfloat16),
            pltpu.VMEM((half, 2 * ROWS, cols), jnp.bfloat16),
            pltpu.VMEM((half, 2 * ROWS, cols), jnp.bfloat16),
            pltpu.VMEM((half, ROWS, cols), jnp.bfloat16),
            pltpu.VMEM((SHARE, ROWS, cols), jnp.bfloat16),
            pltpu.SemaphoreType.DMA((lons // BLOCK,)),
            pltpu.SemaphoreType.DMA((2, steps)),
            pltpu.SemaphoreType.DMA((2, steps)),
            pltpu.SemaphoreType.DMA((lons // BLOCK,)),
            pltpu.SemaphoreType.DMA((lons // BLOCK,)),
            pltpu.SemaphoreType.DMA((4,)),
            pltpu.SemaphoreType.DMA((4,)),
            pltpu.SemaphoreType.DMA((11,)),
            pltpu.SemaphoreType.DMA((11,)),
            pltpu.SemaphoreType.REGULAR,
            pltpu.SemaphoreType.REGULAR,
            pltpu.SemaphoreType.REGULAR,
            pltpu.SemaphoreType.REGULAR,
            pltpu.SemaphoreType.REGULAR,
        ],
        compiler_params=pltpu.CompilerParams(
            collective_id=0, has_side_effects=True, vmem_limit_bytes=40 * 1024 * 1024
        ),
    )(x)
    count = lons - split
    z = pl.pallas_call(
        functools.partial(store, *middle[-1][:2]),
        out_shape=pltpu.HBM((lons, days, cols), jnp.float32),
        in_specs=[pl.BlockSpec(memory_space=pltpu.VMEM)] * 3,
        out_specs=pl.BlockSpec(memory_space=pltpu.HBM),
        scratch_shapes=[
            pltpu.VMEM((count, days, cols), jnp.float32),
            pltpu.VMEM((middle[-1][1], 3 * ROWS, cols), jnp.float32),
            pltpu.SemaphoreType.DMA((-(-split // BLOCK) - (-count // BLOCK),)),
        ],
        compiler_params=pltpu.CompilerParams(vmem_limit_bytes=8 * 1024 * 1024),
    )(
        pltpu.with_memory_space_constraint(held, pltpu.VMEM),
        pltpu.with_memory_space_constraint(anomaly, pltpu.VMEM),
        pltpu.with_memory_space_constraint(far_days, pltpu.VMEM),
    )
    return jnp.transpose(z, (1, 0, 2))


def solution(mesh):
    return jax.shard_map(
        functools.partial(local, (mesh.shape["day"], mesh.shape["lon"])),
        mesh=mesh,
        in_specs=(P("day", "lon", None),),
        out_specs=P("day", "lon", None),
        check_vma=False,
    )
```
